32 devices in a mesh: section: 2 (over y), dp: 4 (over x, core), mp: 4 (over z).
Axes of the slice: x: 2, y: 2, z: 4, core: 2. Of those that a mesh axis runs over, the one named last changes fastest.
Arguments:
- block_input: bfloat16 [2, 4, 1024, 2048], P(None, 'dp', 'mp'), may hold values from -6 to 6
- out_grad: bfloat16 [2, 4, 1024, 2048], P(None, 'dp', 'mp'), may hold values from -6 to 6
- lengths: int32 [2, 4], P(None, 'dp'), may hold values from 1 to 1024, 3072 in all within a row
- norm_gain: float32 [2, 2048], P('section'), may hold values from 0.1 to 1.9
- in_weight: bfloat16 [2, 2048, 2, 4096], P('section', None, None, 'mp'), may hold values from -0.125 to 0.125
- state_weight: bfloat16 [2, 2048, 256], P('section'), may hold values from -0.125 to 0.125
- step_weight: bfloat16 [2, 2048, 64], P('section', None, 'mp'), may hold values from -0.125 to 0.125
- conv_inner: float32 [2, 4, 4096], P('section', None, 'mp'), may hold values from -0.6 to 0.6
- conv_state: float32 [2, 4, 256], P('section'), may hold values from -0.6 to 0.6
- step_bias: float32 [2, 64], P('section', 'mp'), may hold values from -9 to -2
- decay_log: float32 [2, 64], P('section', 'mp'), may hold values from 0 to 2.77
- skip_gain: float32 [2, 64], P('section', 'mp'), may hold values from 0.25 to 2
- gate_gain: float32 [2, 4096], P('section', 'mp'), may hold values from 0.1 to 1.9
- out_weight: bfloat16 [2, 4096, 2048], P('section', 'mp'), may hold values from -0.09375 to 0.09375
Outputs:
- section_out: bfloat16 [2, 2, 4, 1024, 2048], P('section', None, 'dp', 'mp')
- section_in_grad: float32 [2, 2, 4, 1024, 2048], P('section', None, 'dp', 'mp')
- grad_norm_gain: float32 [2, 2048], P('section')
- grad_in_weight: float32 [2, 2048, 2, 4096], P('section', None, None, 'mp')
- grad_state_weight: float32 [2, 2048, 256], P('section')
- grad_step_weight: float32 [2, 2048, 64], P('section', None, 'mp')
- grad_conv_inner: float32 [2, 4, 4096], P('section', None, 'mp')
- grad_conv_state: float32 [2, 4, 256], P('section')
- grad_step_bias: float32 [2, 64], P('section', 'mp')
- grad_decay_log: float32 [2, 64], P('section', 'mp')
- grad_skip_gain: float32 [2, 64], P('section', 'mp')
- grad_gate_gain: float32 [2, 4096], P('section', 'mp')
- grad_out_weight: float32 [2, 4096, 2048], P('section', 'mp')
The draws below stay inside these ranges and needn't reach their ends.
Inputs may be any that keep to these rules, and one draw needn't show every extreme that they name: Each micro-batch's lengths sum to 3072, and the longest of each micro-batch is 1024.
All inputs are finite; a program needn't handle non-finite values. No bound on the sum of `lengths` on one device may be relied on, other than what follows from the above.
Results may differ from the reference program's by a relative error of at most 0.012.
The reference program's roundings to bfloat16 on the way count: a program that leaves them out, or rounds other values in their place, can miss the bound.
Values may be sent and summed in bfloat16 or wider, within the bound.
A program may use at most 320 MiB of HBM per device.

```python
import math
import jax
import jax.numpy as jnp
import numpy as np
from jax import lax

D = 2048
INNER = 4096
HEADS = 64
NSTATE = 128
CONV = 4
BLOCK_LEN = 256
SEQ = 1024
MB = 2
SEQS = 4
SECTIONS = 2


def block_levels(own_key, dims, shards, least, largest):
    loudness, own = 1.0, jax.random.fold_in(own_key, 6)
    for dim, shards_of in shards:
        heights = jnp.exp(jax.random.uniform(jax.random.fold_in(own, dim), (shards_of,), jnp.float32, least / len(shards), largest / len(shards)))
        loudness = loudness * jnp.repeat(heights, dims[dim] // shards_of).reshape([-1 if axis == dim else 1 for axis in range(len(dims))])
    return loudness


def split_up(amount, total, limit, skew):
    loads = [(1 << 20) // math.isqrt(standing ** skew) + 1 for standing in range(2, amount + 1)]
    surplus, holding = total - limit - (amount - 1), [1] * (amount - 1)
    while surplus > 0:
        candidates = [i for i in range(amount - 1) if holding[i] < limit]
        whole, left = sum([loads[i] for i in candidates]), surplus
        for i in candidates:
            more = min(limit - holding[i], max(1, left * loads[i] // whole), surplus)
            holding[i] = holding[i] + more
            surplus = surplus - more
    return np.array([limit] + holding)


def uneven_parts(stream_key, count, total, most, slope):
    if count == 2:
        one = jax.random.randint(stream_key, (), max(1, total - most), min(most, total - 1) + 1)
        return jnp.stack([one, total - one])
    sizes = jnp.asarray(split_up(count, total, most, slope), jnp.int32)
    couples = (count - 1) // 2
    donor, sink = sizes[1:1 + 2 * couples:2], sizes[2:2 + 2 * couples:2]
    room = jnp.minimum(donor - 1, most - sink)
    passed = jax.random.randint(jax.random.fold_in(stream_key, 1), (couples,), 0, 1 << 20) % (room + 1)
    sizes = sizes.at[1:1 + 2 * couples:2].set(donor - passed).at[2:2 + 2 * couples:2].set(sink + passed)
    return sizes[jax.random.permutation(jax.random.fold_in(stream_key, 2), count)]


def gaussian(key, dims, scale, limit, cuts=(), kind=jnp.bfloat16):
    values = jax.random.normal(key, dims, jnp.float32) * scale
    if len(cuts) > 0:
        values = block_levels(key, dims, cuts, -0.22, 0.18) * values
    return jnp.clip(values, min=-limit, max=limit).astype(kind)


def setup_inputs(seed: int = 0) -> dict:
    arg_keys = jax.random.split(jax.random.key(seed), 15)
    block_input = gaussian(arg_keys[0], (MB, SEQS, SEQ, D), 1.0, 6.0, ((1, 4), (2, 4)))
    out_grad = gaussian(arg_keys[1], (MB, SEQS, SEQ, D), 1.0, 6.0, ((1, 4), (2, 4)))
    lengths = jax.vmap(lambda own: uneven_parts(own, SEQS, 3 * SEQ * SEQS // 4, SEQ, 2))(jax.random.split(arg_keys[2], MB)).reshape((MB, SEQS)).astype(jnp.int32)
    norm_gain = jnp.clip(1.0 + 0.18 * jax.random.normal(arg_keys[3], (SECTIONS, D), jnp.float32), 0.1, 1.9)
    in_weight = gaussian(arg_keys[4], (SECTIONS, D, 2, INNER), D ** -0.5, 0.125, ((0, 2), (3, 4)))
    state_weight = gaussian(arg_keys[5], (SECTIONS, D, 2 * NSTATE), D ** -0.5, 0.125, ((0, 2),))
    step_weight = gaussian(arg_keys[6], (SECTIONS, D, HEADS), D ** -0.5, 0.125, ((0, 2), (2, 4)))
    conv_inner = jnp.clip(jax.random.uniform(arg_keys[7], (SECTIONS, CONV, INNER), jnp.float32, -0.6, 0.6) * block_levels(arg_keys[7], (SECTIONS, CONV, INNER), ((0, 2), (2, 4)), -0.4, 0.0), -0.6, 0.6)
    conv_state = jnp.clip(jax.random.uniform(arg_keys[8], (SECTIONS, CONV, 2 * NSTATE), jnp.float32, -0.6, 0.6) * block_levels(arg_keys[8], (SECTIONS, CONV, 2 * NSTATE), ((0, 2),), -0.4, 0.0), -0.6, 0.6)
    step_bias = jnp.clip(-9.0 + 7.0 * jax.random.uniform(arg_keys[9], (SECTIONS, HEADS), jnp.float32) ** block_levels(arg_keys[9], (SECTIONS, HEADS), ((0, 2), (1, 4)), -0.2, 0.2), -9.0, -2.0)
    decay_log = jnp.clip(2.77 * jax.random.uniform(arg_keys[10], (SECTIONS, HEADS), jnp.float32) ** block_levels(arg_keys[10], (SECTIONS, HEADS), ((0, 2), (1, 4)), -0.2, 0.2), 0.0, 2.77)
    skip_gain = jnp.clip(0.25 + 1.75 * jax.random.uniform(arg_keys[11], (SECTIONS, HEADS), jnp.float32) ** block_levels(arg_keys[11], (SECTIONS, HEADS), ((0, 2), (1, 4)), -0.2, 0.2), 0.25, 2.0)
    gate_gain = jnp.clip(1.0 + 0.18 * jax.random.normal(arg_keys[12], (SECTIONS, INNER), jnp.float32), 0.1, 1.9)
    out_weight = gaussian(arg_keys[13], (SECTIONS, INNER, D), INNER ** -0.5, 0.09375, ((0, 2), (1, 4)))
    return dict(block_input=block_input, out_grad=out_grad, lengths=lengths, norm_gain=norm_gain, in_weight=in_weight, state_weight=state_weight, step_weight=step_weight, conv_inner=conv_inner, conv_state=conv_state, step_bias=step_bias, decay_log=decay_log, skip_gain=skip_gain, gate_gain=gate_gain, out_weight=out_weight)


@jax.custom_vjp
def low(v):
    return lax.optimization_barrier(v.astype(jnp.bfloat16)).astype(jnp.float32)

@jax.custom_vjp
def low_back(v):
    return v

def low_keep(v):
    return (low(v), None)

def low_pass(kept, grad):
    return (grad,)

def back_keep(v):
    return (v, None)

def back_low(kept, grad):
    return (low(grad),)
low.defvjp(low_keep, low_pass)
low_back.defvjp(back_keep, back_low)
epsilon = 1e-05
highest = lax.Precision.HIGHEST

def causal_conv(series, kernel):
    taps = kernel.shape[0]
    length = series.shape[0]
    padded = jnp.concatenate([jnp.zeros((taps - 1, series.shape[1]), jnp.float32), series], axis=0)
    summed = jnp.zeros_like(series)
    for offset in range(taps):
        summed = summed + kernel[offset] * padded[offset:offset + length]
    return summed

def state_scan(head_inputs, b_matrix, c_matrix, step_size, decay_rates, skip_gain):
    length, head_count, head_width = head_inputs.shape
    block_count = length // BLOCK_LEN
    x_blocks = head_inputs.reshape(block_count, BLOCK_LEN, head_count, head_width)
    b_blocks = b_matrix.reshape(block_count, BLOCK_LEN, -1)
    c_blocks = c_matrix.reshape(block_count, BLOCK_LEN, -1)
    step_blocks = step_size.reshape(block_count, BLOCK_LEN, head_count)
    log_decay = -jnp.cumsum(step_blocks * decay_rates, axis=1)
    scores = jnp.einsum('ktn,ksn->kts', c_blocks, b_blocks, precision=highest)
    ahead = jnp.arange(BLOCK_LEN)[:, None] >= jnp.arange(BLOCK_LEN)[None, :]
    causal = ahead[None, :, :, None]
    log_gap = log_decay[:, :, None, :] - log_decay[:, None, :, :]
    weights = jnp.where(causal, jnp.exp(jnp.where(causal, log_gap, 0.0)), 0.0)
    weights = weights * scores[:, :, :, None] * step_blocks[:, None, :, :]
    within = jnp.einsum('ktsh,kshp->kthp', weights, x_blocks, precision=highest)
    tail_decay = jnp.exp(log_decay[:, -1:, :] - log_decay) * step_blocks
    states = jnp.einsum('ksn,kshp->khnp', b_blocks, x_blocks * tail_decay[:, :, :, None], precision=highest)
    carried = jnp.zeros(states.shape[1:], jnp.float32)
    entering = []
    for block_index in range(block_count):
        entering.append(carried)
        carried = jnp.exp(log_decay[block_index, -1])[:, None, None] * carried + states[block_index]
    entering = jnp.stack(entering)
    cross = jnp.einsum('ktn,khnp->kthp', c_blocks, entering, precision=highest) * jnp.exp(log_decay)[:, :, :, None]
    result = within + cross + skip_gain[None, None, :, None] * x_blocks
    return result.reshape(length, head_count, head_width)

def mixer_layer(rows, mask_rows, norm_gain, in_weight, state_weight, step_weight, conv_inner, conv_state, step_bias, decay_log, skip_gain, gate_gain, out_weight):
    seq_count, length, model_width = rows.shape
    inner_width = in_weight.shape[2]
    head_count = step_bias.shape[0]
    state_width = state_weight.shape[1] // 2
    flat_rows = rows.reshape(seq_count * length, model_width)
    row_scale = lax.rsqrt(lax.optimization_barrier(jnp.mean(flat_rows * flat_rows, axis=1, keepdims=True)) + epsilon)
    normal = low(flat_rows * row_scale * norm_gain)
    gate_pre = low_back(jnp.dot(normal, in_weight[:, 0], precision=highest))
    inner_pre = low_back(jnp.dot(normal, in_weight[:, 1], precision=highest))
    state_pre = low_back(jnp.dot(normal, state_weight, precision=highest))
    step_pre = low_back(jnp.dot(normal, step_weight, precision=highest))
    conv_all = jax.vmap(causal_conv, in_axes=(0, None))
    inner_act = low(jax.nn.silu(conv_all(inner_pre.reshape(seq_count, length, inner_width), conv_inner)))
    state_act = low(jax.nn.silu(conv_all(state_pre.reshape(seq_count, length, 2 * state_width), conv_state)))
    step_size = jax.nn.softplus(step_pre.reshape(seq_count, length, head_count) + step_bias)
    decay_rates = jnp.exp(decay_log)

    def one_sequence(sequence_item):
        head_inputs, state_values, step_values = sequence_item
        return state_scan(head_inputs, state_values[:, :state_width], state_values[:, state_width:], step_values, decay_rates, skip_gain)
    mixed = lax.map(jax.checkpoint(one_sequence), (inner_act.reshape(seq_count, length, head_count, inner_width // head_count), state_act, step_size))
    gated_out = mixed.reshape(seq_count * length, inner_width) * jax.nn.silu(gate_pre)
    inv_rms = lax.rsqrt(lax.optimization_barrier(jnp.mean(gated_out * gated_out, axis=1, keepdims=True)) + epsilon)
    normed = low(gated_out * inv_rms * gate_gain)
    branch = low_back(jnp.dot(normed, out_weight, precision=highest))
    result = flat_rows + mask_rows.reshape(-1, 1) * branch
    return low(low_back(result)).reshape(seq_count, length, model_width)

def reference(block_input, out_grad, lengths, norm_gain, in_weight, state_weight, step_weight, conv_inner, conv_state, step_bias, decay_log, skip_gain, gate_gain, out_weight):
    positions = jnp.arange(SEQ, dtype=jnp.int32)
    section_params = []
    for section_id in range(SECTIONS):
        section_params.append((norm_gain[section_id], in_weight[section_id].astype(jnp.float32), state_weight[section_id].astype(jnp.float32), step_weight[section_id].astype(jnp.float32), conv_inner[section_id], conv_state[section_id], step_bias[section_id], decay_log[section_id], skip_gain[section_id], gate_gain[section_id], out_weight[section_id].astype(jnp.float32)))
    totals = [jax.tree.map(jnp.zeros_like, params) for params in section_params]
    first_outs, second_outs, first_grads, second_grads = ([], [], [], [])
    for micro_index in range(MB):
        mask_rows = (positions[None, :] < lengths[micro_index][:, None]).astype(jnp.float32)

        def layer_apply(rows, *params):
            return mixer_layer(rows, mask_rows, *params)
        hidden, first_pull = jax.vjp(layer_apply, block_input[micro_index].astype(jnp.float32), *section_params[0])
        final, second_pull = jax.vjp(layer_apply, hidden, *section_params[1])
        second_back = second_pull(out_grad[micro_index].astype(jnp.float32))
        first_back = first_pull(second_back[0])
        totals[0] = jax.tree.map(lambda left, right: left + right, totals[0], tuple(first_back[1:]))
        totals[1] = jax.tree.map(lambda left, right: left + right, totals[1], tuple(second_back[1:]))
        first_outs.append(hidden)
        second_outs.append(final)
        first_grads.append(first_back[0])
        second_grads.append(second_back[0])
    section_out = jnp.stack([jnp.stack(first_outs), jnp.stack(second_outs)]).astype(jnp.bfloat16)
    section_in_grad = jnp.stack([jnp.stack(first_grads), jnp.stack(second_grads)])
    stacked = [jnp.stack([totals[0][number], totals[1][number]]) for number in range(11)]
    return (section_out, section_in_grad, stacked[0], stacked[1], stacked[2], stacked[3], stacked[4], stacked[5], stacked[6], stacked[7], stacked[8], stacked[9], stacked[10])
```

```python
import functools
import jax
import jax.numpy as jnp
from jax import lax
from jax.experimental import pallas as pl
from jax.experimental.pallas import tpu as pltpu
from jax.sharding import PartitionSpec as P

epsilon = 1e-05
f32 = jnp.float32
bf16 = jnp.bfloat16
highest = lax.Precision.HIGHEST
BLOCK = 256
HALO = 8
LOG2E = 1.4426950408889634


def mm(a, b, contract, precision=None):
    return lax.dot_general(a, b, (contract, ((), ())), preferred_element_type=f32, precision=precision)


NN = ((1,), (0,))
NT = ((1,), (1,))
TN = ((0,), (0,))


def sigmoid(v):
    return 0.5 * jnp.tanh(0.5 * v) + 0.5


def step_of(z):
    e = jnp.exp(-jnp.abs(z))
    u = 1.0 + e
    d = u - 1.0
    tail = jnp.where(d == 0.0, e, jnp.log(u) * (e / jnp.where(d == 0.0, 1.0, d)))
    return jnp.maximum(z, 0.0) + tail


def triangle(inclusive, upper=False):
    r = lax.broadcasted_iota(jnp.int32, (BLOCK, BLOCK), 0)
    c = lax.broadcasted_iota(jnp.int32, (BLOCK, BLOCK), 1)
    if upper:
        r, c = c, r
    return (r >= c) if inclusive else (r > c)


def pad_lanes(v, to=128):
    return jnp.concatenate([v, jnp.zeros((v.shape[0], to - v.shape[1]), v.dtype)], axis=1)


def low_half(shape):
    return lax.broadcasted_iota(jnp.int32, shape, 1) < 64


def pair_of(cols, p):
    rows = cols.shape[0]
    lo = low_half((rows, 128))
    return jnp.where(lo, cols[:, 2 * p : 2 * p + 1], cols[:, 2 * p + 1 : 2 * p + 2])


def block_setup(step_pre, bias, decay, heads):
    z = step_pre + bias
    step = step_of(z)
    rate = jnp.exp(decay)
    dec = pad_lanes(step * rate)
    tri = triangle(True).astype(f32)
    ld = -mm(tri, dec, NN, highest)[:, :heads]
    return z, step, rate, ld


def fwd_kernel(sizes, pre, taps, heads3, gain, mixed, scaled, sq, states, ext, carry, scr):
    inner, state, heads = sizes
    k = pl.program_id(0)
    nst = state // 2
    pairs = heads // 2
    a_state, a_step = 2 * inner, 2 * inner + state

    @pl.when(k == 0)
    def _():
        ext[0:HALO, :] = jnp.zeros((HALO, inner + state), f32)
        carry[...] = jnp.zeros_like(carry)

    ext[HALO:, :] = pre[:, inner:a_step]

    def act(lo, width):
        c = taps[0:1, lo : lo + width] * ext[HALO - 3 : HALO - 3 + BLOCK, lo : lo + width]
        for j in range(1, 4):
            c = c + taps[j : j + 1, lo : lo + width] * ext[HALO - 3 + j : HALO - 3 + j + BLOCK, lo : lo + width]
        return (c * sigmoid(c)).astype(bf16)

    b = act(inner, nst)
    c = act(inner + nst, nst)
    z, step, rate, ld = block_setup(pre[:, a_step : a_step + heads], heads3[0:1, :heads], heads3[1:2, :heads], heads)
    ld2 = ld * LOG2E
    rrow = jnp.transpose(pad_lanes(jnp.log2(step) - ld2))
    eld = jnp.exp2(ld2)
    last = ld2[BLOCK - 1 : BLOCK, :]
    tail = jnp.exp2(last - ld2) * step
    scr[...] = jnp.where(triangle(True), mm(c, b, NT), 0.0)
    squares = jnp.zeros((BLOCK, 1), f32)
    half = BLOCK // 2
    for p in range(pairs):
        lanes = slice(128 * p, 128 * p + 128)
        x = act(128 * p, 128)
        xf = x.astype(f32)
        lo = low_half((BLOCK, 128))
        xs = [jnp.where(lo, x, jnp.zeros_like(x)), jnp.where(lo, jnp.zeros_like(x), x)]
        tops, bottoms = [], []
        for i in range(2):
            h = 2 * p + i
            top = jnp.exp2(jnp.minimum(ld2[:half, h : h + 1] + rrow[h : h + 1, :half], 40.0)) * scr[:half, :half]
            tops.append(mm(top.astype(bf16), xs[i][:half], NN))
            bot = jnp.exp2(jnp.minimum(ld2[half:, h : h + 1] + rrow[h : h + 1, :], 40.0)) * scr[half:, :]
            bottoms.append(mm(bot.astype(bf16), xs[i], NN))
        within = jnp.concatenate([tops[0] + tops[1], bottoms[0] + bottoms[1]], axis=0)
        s_in = carry[:, lanes]
        e_pair = pair_of(eld, p)
        cross = mm(c, s_in.astype(bf16), NN) * e_pair
        y = within + cross + pair_of(heads3[2:3, :heads], p) * xf
        mixed[:, lanes] = y
        g = pre[:, lanes]
        gated = y * (g * sigmoid(g))
        squares = squares + jnp.sum(gated * gated, axis=1, keepdims=True)
        scaled[:, lanes] = (gated * gain[:, lanes]).astype(bf16)
        s_out = e_pair[BLOCK - 1 :, :] * s_in + mm(b, (xf * pair_of(tail, p)).astype(bf16), TN)
        carry[:, lanes] = s_out
        states[0, :, lanes] = s_out
    sq[...] = squares
    ext[0:HALO, :] = ext[BLOCK : BLOCK + HALO, :]


def mix_forward(pre, taps, heads3, gain, inner, state, heads):
    rows = pre.shape[0]
    blocks = rows // BLOCK
    width = pre.shape[1]
    nst = state // 2
    return pl.pallas_call(
        functools.partial(fwd_kernel, (inner, state, heads)),
        grid=(blocks,),
        in_specs=[
            pl.BlockSpec((BLOCK, width), lambda k: (k, 0)),
            pl.BlockSpec((4, inner + state), lambda k: (0, 0)),
            pl.BlockSpec((3, heads), lambda k: (0, 0)),
            pl.BlockSpec((1, inner), lambda k: (0, 0)),
        ],
        out_specs=[
            pl.BlockSpec((BLOCK, inner), lambda k: (k, 0)),
            pl.BlockSpec((BLOCK, inner), lambda k: (k, 0)),
            pl.BlockSpec((BLOCK, 1), lambda k: (k, 0)),
            pl.BlockSpec((1, nst, inner), lambda k: (k, 0, 0)),
        ],
        out_shape=[
            jax.ShapeDtypeStruct((rows, inner), f32),
            jax.ShapeDtypeStruct((rows, inner), bf16),
            jax.ShapeDtypeStruct((rows, 1), f32),
            jax.ShapeDtypeStruct((blocks, nst, inner), f32),
        ],
        scratch_shapes=[
            pltpu.VMEM((BLOCK + HALO, inner + state), f32),
            pltpu.VMEM((nst, inner), f32),
            pltpu.VMEM((BLOCK, BLOCK), f32),
        ],
        name="mix_forward",
    )(pre, taps, heads3, gain)


def bwd_kernel(sizes, pre, halo, mixed, ngrad, rows2, s_in_ref, taps, heads3, gain,
               own, normed, g_taps, g_heads, g_gain, ext, dext, carry, acc, scr, dyb, xb, cold, rowd, xw):
    inner, state, heads = sizes
    step_id = pl.program_id(0)
    blocks = pl.num_programs(0)
    k = blocks - 1 - step_id
    nst = state // 2
    pairs = heads // 2
    a_state, a_step = 2 * inner, 2 * inner + state

    @pl.when(step_id == 0)
    def _():
        dext[BLOCK:, :] = jnp.zeros((HALO, inner + state), f32)
        carry[...] = jnp.zeros_like(carry)
        g_taps[...] = jnp.zeros_like(g_taps)
        g_heads[...] = jnp.zeros_like(g_heads)
        g_gain[...] = jnp.zeros_like(g_gain)

    ext[HALO:, :] = pre[:, inner:a_step]
    ext[0:HALO, :] = jnp.where(k == 0, 0.0, halo[:, inner:a_step])

    def conv(lo, width):
        c = taps[0:1, lo : lo + width] * ext[HALO - 3 : HALO - 3 + BLOCK, lo : lo + width]
        for j in range(1, 4):
            c = c + taps[j : j + 1, lo : lo + width] * ext[HALO - 3 + j : HALO - 3 + j + BLOCK, lo : lo + width]
        return c

    def dsilu(v):
        s = sigmoid(v)
        return s * (1.0 + v * (1.0 - s))

    cb = conv(inner, nst)
    cc = conv(inner + nst, nst)
    b = (cb * sigmoid(cb)).astype(bf16)
    c = (cc * sigmoid(cc)).astype(bf16)
    z, step, rate, ld = block_setup(pre[:, a_step : a_step + heads], heads3[0:1, :heads], heads3[1:2, :heads], heads)
    ld2 = ld * LOG2E
    ldrow = jnp.transpose(pad_lanes(ld2))
    rcol = jnp.log2(step) - ld2
    eld = jnp.exp2(ld2)
    tail = jnp.exp2(ld2[BLOCK - 1 : BLOCK, :] - ld2) * step
    scr[...] = jnp.where(triangle(True, upper=True), mm(b, c, NT), 0.0)
    acc[...] = jnp.zeros_like(acc)
    half = BLOCK // 2
    inv = rows2[:, 0:1]
    pull = rows2[:, 1:2]
    d_b = jnp.zeros((BLOCK, nst), f32)
    d_c = jnp.zeros((BLOCK, nst), f32)
    head_lane = lax.broadcasted_iota(jnp.int32, (1, 128), 1)
    cold[...] = jnp.zeros_like(cold)
    xw[...] = jnp.zeros_like(xw)
    carried = jnp.zeros((1, 128), f32)
    skips = jnp.zeros((1, 128), f32)
    for p in range(pairs):
        lanes = slice(128 * p, 128 * p + 128)
        lo = low_half((BLOCK, 128))
        lo1 = low_half((1, 128))
        g = pre[:, lanes]
        sg = sigmoid(g)
        silu = g * sg
        y = mixed[:, lanes]
        gated = y * silu
        ng = ngrad[:, lanes]
        gn = gain[:, lanes]
        gi = gated * inv
        normed[:, lanes] = (gi * gn).astype(bf16)
        g_gain[:, lanes] += jnp.sum(ng * gi, axis=0, keepdims=True)
        gg = inv * (ng * gn) - gated * pull
        own[:, lanes] = (gg * y * (sg * (1.0 + g * (1.0 - sg)))).astype(bf16)
        dy = gg * silu
        cx = conv(128 * p, 128)
        sx = sigmoid(cx)
        x = (cx * sx).astype(bf16)
        xf = x.astype(f32)
        dyh = dy.astype(bf16)
        zero = jnp.zeros_like(x)
        xs = [jnp.where(lo, x, zero), jnp.where(lo, zero, x)]
        dys = [jnp.where(lo, dyh, zero), jnp.where(lo, zero, dyh)]
        tops, bottoms = [], []
        for i in range(2):
            h = 2 * p + i
            w_top = jnp.exp2(jnp.minimum(ldrow[h : h + 1, :] + rcol[:half, h : h + 1], 40.0))
            s_top = scr[:half, :]
            m_top = w_top * s_top
            tops.append(mm(m_top.astype(bf16), dys[i], NN))
            gm = mm(xs[i][:half], dyh, NT) * w_top
            acc[:half, :] += gm
            e_top = gm * s_top
            w_bot = jnp.exp2(jnp.minimum(ldrow[h : h + 1, half:] + rcol[half:, h : h + 1], 40.0))
            s_bot = scr[half:, half:]
            m_bot = w_bot * s_bot
            bottoms.append(mm(m_bot.astype(bf16), dys[i][half:], NN))
            gm = mm(xs[i][half:], dyh[half:], NT) * w_bot
            acc[half:, half:] += gm
            e_bot = gm * s_bot
            cold[:half, h : h + 1] = jnp.sum(e_top, axis=1, keepdims=True)
            cold[half:, h : h + 1] = jnp.sum(e_bot, axis=1, keepdims=True)
            top_row = jnp.sum(e_top, axis=0, keepdims=True)
            rowd[h : h + 1, :half] = top_row[:, :half]
            rowd[h : h + 1, half:] = top_row[:, half:] + jnp.sum(e_bot, axis=0, keepdims=True)
        dxm = jnp.concatenate([tops[0] + tops[1], bottoms[0] + bottoms[1]], axis=0)
        ds = carry[:, lanes]
        dsh = ds.astype(bf16)
        s_in = jnp.where(k == 0, 0.0, s_in_ref[0, :, lanes])
        s_h = s_in.astype(bf16)
        e_pair = pair_of(eld, p)
        t_pair = pair_of(tail, p)
        dye = (dy * e_pair).astype(bf16)
        cross = mm(c, s_h, NN) * e_pair * dy
        w = mm(b, dsh, NN) * t_pair
        wx = w * xf
        for i in range(2):
            h = 2 * p + i
            keep = lo if i == 0 else jnp.logical_not(lo)
            xw[:, h : h + 1] = jnp.sum(jnp.where(keep, wx, 0.0), axis=1, keepdims=True)
            xw[:, 64 + h : 65 + h] = jnp.sum(jnp.where(keep, cross, 0.0), axis=1, keepdims=True)
        d_c = d_c + mm(dye, s_h, NT)
        d_b = d_b + mm((xf * t_pair).astype(bf16), dsh, NT)
        skip_pair = pair_of(heads3[2:3, :heads], p)
        dx = dxm + skip_pair * dy + w
        dskip = jnp.sum(dy * xf, axis=0, keepdims=True)
        dstate = jnp.sum(ds * s_in, axis=0, keepdims=True) * e_pair[BLOCK - 1 :, :]
        for i in range(2):
            h = 2 * p + i
            keep = lo1 if i == 0 else jnp.logical_not(lo1)
            skips = jnp.where(head_lane == h, jnp.sum(jnp.where(keep, dskip, 0.0), axis=1, keepdims=True), skips)
            carried = jnp.where(head_lane == h, jnp.sum(jnp.where(keep, dstate, 0.0), axis=1, keepdims=True), carried)
        carry[:, lanes] = e_pair[BLOCK - 1 :, :] * ds + mm(c, dye, TN)
        dext[:BLOCK, lanes] = dx * (sx * (1.0 + cx * (1.0 - sx)))
    ah = jnp.where(triangle(True, upper=True), acc[...], 0.0).astype(bf16)
    d_b = d_b + mm(ah, c, NN)
    d_c = d_c + mm(ah, b, TN)
    dext[:BLOCK, inner : inner + nst] = d_b * dsilu(cb)
    dext[:BLOCK, inner + nst :] = d_c * dsilu(cc)
    colsum = cold[...]
    rowsum = jnp.transpose(jnp.concatenate([rowd[...], jnp.zeros((128 - heads, BLOCK), f32)], axis=0))
    xwv = xw[...]
    crossv = pltpu.roll(xwv, 64, 1)
    lane = lax.broadcasted_iota(jnp.int32, (BLOCK, 128), 1)
    tailv = jnp.where(lane < heads, xwv, 0.0)
    crossv = jnp.where(lane < heads, crossv, 0.0)
    upper = triangle(True, upper=True).astype(f32)
    strict = triangle(False).astype(f32)
    from_q = mm(upper, rowsum - colsum + crossv, NN, highest) + mm(strict, tailv, NN, highest) + carried
    ddec = -from_q[:, :heads]
    q = (colsum + tailv)[:, :heads]
    sz = sigmoid(z)
    ratio = jnp.where(step > 1e-30, sz / jnp.where(step > 1e-30, step, 1.0), 1.0)
    dz = q * ratio + rate * ddec * sz
    own[:, a_step : a_step + heads] = dz.astype(bf16)
    g_heads[0:1, :heads] += jnp.sum(dz, axis=0, keepdims=True)
    g_heads[1:2, :heads] += rate * jnp.sum(step * ddec, axis=0, keepdims=True)
    g_heads[2:3, :] += skips
    for at in range(0, inner + state, 256):
        lanes = slice(at, at + 256)
        dpre = taps[3:4, lanes] * dext[0:BLOCK, lanes]
        for j in range(3):
            dpre = dpre + taps[j : j + 1, lanes] * dext[3 - j : 3 - j + BLOCK, lanes]
        own[:, inner + at : inner + at + 256] = dpre.astype(bf16)
        d = dext[0:BLOCK, lanes]
        for j in range(4):
            g_taps[j : j + 1, lanes] += jnp.sum(d * ext[HALO - 3 + j : HALO - 3 + j + BLOCK, lanes], axis=0, keepdims=True)
    dext[BLOCK:, :] = dext[0:HALO, :]


def mix_backward(pre, mixed, ngrad, rows2, states, taps, heads3, gain, inner, state, heads):
    rows = pre.shape[0]
    blocks = rows // BLOCK
    width = pre.shape[1]
    nst = state // 2
    last = blocks - 1
    per = BLOCK // HALO
    return pl.pallas_call(
        functools.partial(bwd_kernel, (inner, state, heads)),
        grid=(blocks,),
        in_specs=[
            pl.BlockSpec((BLOCK, width), lambda k: (last - k, 0)),
            pl.BlockSpec((HALO, width), lambda k: (jnp.maximum((last - k) * per - 1, 0), 0)),
            pl.BlockSpec((BLOCK, inner), lambda k: (last - k, 0)),
            pl.BlockSpec((BLOCK, inner), lambda k: (last - k, 0)),
            pl.BlockSpec((BLOCK, 2), lambda k: (last - k, 0)),
            pl.BlockSpec((1, nst, inner), lambda k: (jnp.maximum(last - k - 1, 0), 0, 0)),
            pl.BlockSpec((4, inner + state), lambda k: (0, 0)),
            pl.BlockSpec((3, heads), lambda k: (0, 0)),
            pl.BlockSpec((1, inner), lambda k: (0, 0)),
        ],
        out_specs=[
            pl.BlockSpec((BLOCK, width), lambda k: (last - k, 0)),
            pl.BlockSpec((BLOCK, inner), lambda k: (last - k, 0)),
            pl.BlockSpec((4, inner + state), lambda k: (0, 0)),
            pl.BlockSpec((8, 128), lambda k: (0, 0)),
            pl.BlockSpec((1, inner), lambda k: (0, 0)),
        ],
        out_shape=[
            jax.ShapeDtypeStruct((rows, width), bf16),
            jax.ShapeDtypeStruct((rows, inner), bf16),
            jax.ShapeDtypeStruct((4, inner + state), f32),
            jax.ShapeDtypeStruct((8, 128), f32),
            jax.ShapeDtypeStruct((1, inner), f32),
        ],
        scratch_shapes=[
            pltpu.VMEM((BLOCK + HALO, inner + state), f32),
            pltpu.VMEM((BLOCK + HALO, inner + state), f32),
            pltpu.VMEM((nst, inner), f32),
            pltpu.VMEM((BLOCK, BLOCK), f32),
            pltpu.VMEM((BLOCK, BLOCK), f32),
            pltpu.VMEM((8, 128), f32),
            pltpu.VMEM((8, 128), f32),
            pltpu.VMEM((BLOCK, 128), f32),
            pltpu.VMEM((heads, BLOCK), f32),
            pltpu.VMEM((BLOCK, 128), f32),
        ],
        name="mix_backward",
    )(pre, pre, mixed, ngrad, rows2, states, taps, heads3, gain)


def on_device(
    block_input,
    out_grad,
    lengths,
    norm_gain,
    in_weight,
    state_weight,
    step_weight,
    conv_inner,
    conv_state,
    step_bias,
    decay_log,
    skip_gain,
    gate_gain,
    out_weight,
):
    sections = lax.axis_size("section")
    section_id = lax.axis_index("section")
    dp_count = lax.axis_size("dp")
    dp_index = lax.axis_index("dp")
    part_count = lax.axis_size("mp")
    part_index = lax.axis_index("mp")
    row_count, model_width = block_input.shape[2:]
    inner_local = in_weight.shape[3]
    inner_total = inner_local * part_count
    state_width = state_weight.shape[2]
    heads_local = step_weight.shape[2]
    first = section_id == 0
    swap = [(0, 1), (1, 0)]

    rows_in = lax.dynamic_index_in_dim(block_input[:, 0], section_id, 0, keepdims=False)
    outer_grad = lax.dynamic_index_in_dim(out_grad[:, 0], section_id, 0, keepdims=False)
    live = lax.dynamic_index_in_dim(lengths[:, 0], section_id, 0, keepdims=False)
    positions = part_index * row_count + jnp.arange(row_count, dtype=jnp.int32)
    mask = (positions < live).astype(f32)[:, None]

    small_shapes = [norm_gain.shape, conv_inner.shape, conv_state.shape, step_bias.shape, decay_log.shape, skip_gain.shape, gate_gain.shape]
    packed = jnp.concatenate([v.reshape(-1) for v in (norm_gain, conv_inner, conv_state, step_bias, decay_log, skip_gain, gate_gain)])
    packed = lax.all_gather(packed, "section")
    smalls = []
    for layer in range(sections):
        at, pieces = 0, []
        for shape in small_shapes:
            size = 1
            for s in shape:
                size *= s
            pieces.append(packed[layer, at : at + size].reshape(shape[1:]))
            at += size
        smalls.append(
            (
                pieces[0],
                jnp.concatenate([pieces[1], pieces[2]], axis=1),
                jnp.stack(pieces[3:6]),
                pieces[6].reshape(1, -1),
            )
        )

    def other_section(weight):
        quarter = weight.shape[0] // dp_count
        mine = lax.dynamic_slice_in_dim(weight, dp_index * quarter, quarter, 0)
        theirs = lax.ppermute(mine, "section", swap)
        return lax.all_gather(theirs, "dp", axis=0, tiled=True)

    own_in = jnp.concatenate([in_weight[0, :, 0], in_weight[0, :, 1], state_weight[0], step_weight[0]], axis=1)
    own_out = out_weight[0]
    other_in = other_section(own_in)
    other_out = other_section(own_out)
    weights = [
        (jnp.where(first, own_in, other_in), jnp.where(first, own_out, other_out)),
        (jnp.where(first, other_in, own_in), jnp.where(first, other_out, own_out)),
    ]
    at_inner, at_state, at_step = inner_local, 2 * inner_local, 2 * inner_local + state_width

    def forward(layer, values):
        w_in, w_out = weights[layer]
        gain_norm, taps, heads3, gain_gate = smalls[layer]
        row_scale = lax.rsqrt(jnp.mean(values * values, axis=1, keepdims=True) + epsilon)
        normal = (values * row_scale * gain_norm).astype(bf16)
        gathered = lax.all_gather(normal, "mp", axis=0, tiled=True)
        pre = jnp.dot(gathered, w_in, preferred_element_type=f32)
        mixed, scaled, sq, states = mix_forward(pre, taps, heads3, gain_gate, inner_local, state_width, heads_local)
        squares = lax.psum_scatter(sq[:, 0], "mp", scatter_dimension=0, tiled=True)
        inv_rms = lax.rsqrt(squares / inner_total + epsilon)[:, None]
        part = jnp.dot(scaled, w_out, preferred_element_type=f32).astype(bf16)
        branch = lax.psum_scatter(part, "mp", scatter_dimension=0, tiled=True).astype(f32) * inv_rms
        result = (values + mask * branch).astype(bf16)
        return result, (values, row_scale, gathered, pre, mixed, states, inv_rms, branch)

    def backward(layer, kept, grad):
        w_in, w_out = weights[layer]
        gain_norm, taps, heads3, gain_gate = smalls[layer]
        values, row_scale, gathered, pre, mixed, states, inv_own, branch = kept
        branch_grad = (mask * grad).astype(bf16)
        pull_own = inv_own * inv_own * jnp.sum(branch_grad.astype(f32) * branch, axis=1, keepdims=True) / inner_total
        scalars = lax.all_gather(jnp.concatenate([inv_own, pull_own], axis=1), "mp", axis=0, tiled=True)
        full_grad = lax.all_gather(branch_grad, "mp", axis=0, tiled=True)
        normed_grad = jnp.einsum("ld,id->li", full_grad, w_out, preferred_element_type=f32)
        own_grad, normed, g_taps, g_heads, g_gain = mix_backward(
            pre, mixed, normed_grad, scalars, states, taps, heads3, gain_gate, inner_local, state_width, heads_local
        )
        out_part = jnp.einsum("li,ld->id", normed, full_grad, preferred_element_type=f32)
        in_part = jnp.einsum("ld,lc->dc", gathered, own_grad, preferred_element_type=f32)
        part = jnp.einsum("lc,dc->ld", own_grad, w_in, preferred_element_type=f32).astype(bf16)
        normal_grad = lax.psum_scatter(part, "mp", scatter_dimension=0, tiled=True).astype(f32)
        norm_part = jnp.sum(normal_grad * values * row_scale, axis=0)
        scaled_in = normal_grad * gain_norm
        input_grad = (
            grad
            + row_scale * scaled_in
            - values * row_scale**3 * jnp.mean(scaled_in * values, axis=1, keepdims=True)
        )
        own_small = (g_taps[:, :inner_local], g_heads[0, :heads_local], g_heads[1, :heads_local], g_heads[2, :heads_local], g_gain[0])
        common_small = (norm_part, g_taps[:, inner_local:])
        return input_grad, in_part.astype(bf16), out_part.astype(bf16), own_small, common_small

    def spread(part):
        return lax.psum_scatter(part, "dp", scatter_dimension=0, tiled=True)

    hidden, kept_first = forward(0, rows_in.astype(f32))
    final, kept_second = forward(1, hidden.astype(f32))
    second_grad, in_second, out_second, own_second, common_second = backward(1, kept_second, outer_grad.astype(f32))
    first_grad, in_first, out_first, own_first, common_first = backward(0, kept_first, second_grad.astype(bf16).astype(f32))

    out_second, in_second = spread(out_second), spread(in_second)
    out_first, in_first = spread(out_first), spread(in_first)

    def to_owner(part_first, part_second):
        mine = jnp.where(first, part_first, part_second).astype(f32)
        theirs = jnp.where(first, part_second, part_first)
        total = (mine + lax.ppermute(theirs, "section", swap).astype(f32)).astype(bf16)
        return total

    out_total = lax.all_gather(to_owner(out_first, out_second), "dp", axis=0, tiled=True)
    in_quarter = to_owner(in_first, in_second)
    state_quarter = lax.psum(in_quarter[:, at_state:at_step].astype(f32), "mp").astype(bf16)
    in_total = lax.all_gather(in_quarter, "dp", axis=0, tiled=True)
    state_total = lax.all_gather(state_quarter, "dp", axis=0, tiled=True)

    def flat(pieces):
        return jnp.concatenate([v.reshape(-1) for v in pieces])

    own_sum = lax.psum(jnp.stack([flat(own_first), flat(own_second)]), ("section", "dp"))
    common_sum = lax.psum(jnp.stack([flat(common_first), flat(common_second)]), ("section", "dp", "mp"))
    own_sum = lax.dynamic_index_in_dim(own_sum, section_id, 0, keepdims=False)
    common_sum = lax.dynamic_index_in_dim(common_sum, section_id, 0, keepdims=False)

    def cut(vector, shapes):
        at, pieces = 0, []
        for shape in shapes:
            size = 1
            for s in shape:
                size *= s
            pieces.append(vector[at : at + size].reshape((1,) + tuple(shape)))
            at += size
        return pieces

    g_conv_inner, g_bias, g_decay, g_skip, g_gate_gain = cut(own_sum, [v.shape for v in own_first])
    g_norm, g_conv_state = cut(common_sum, [v.shape for v in common_first])

    def by_section(of_first, of_second):
        mine = jnp.where(first, of_first, of_second)
        theirs = lax.ppermute(jnp.where(first, of_second, of_first).astype(bf16), "section", swap).astype(mine.dtype)
        return jnp.where(first, jnp.stack([mine, theirs]), jnp.stack([theirs, mine]))[None, :, None]

    in_total = in_total.astype(f32)
    return (
        by_section(hidden, final),
        by_section(first_grad, second_grad),
        g_norm,
        jnp.stack([in_total[:, :at_inner], in_total[:, at_inner:at_state]], axis=1)[None],
        state_total.astype(f32)[None],
        in_total[:, at_step:][None],
        g_conv_inner,
        g_conv_state,
        g_bias,
        g_decay,
        g_skip,
        g_gate_gain,
        out_total.astype(f32)[None],
    )


def solution(mesh):
    return jax.shard_map(
        on_device,
        mesh=mesh,
        in_specs=(
            P(None, "dp", "mp", None),
            P(None, "dp", "mp", None),
            P(None, "dp"),
            P("section", None),
            P("section", None, None, "mp"),
            P("section", None, None),
            P("section", None, "mp"),
            P("section", None, "mp"),
            P("section", None, None),
            P("section", "mp"),
            P("section", "mp"),
            P("section", "mp"),
            P("section", "mp"),
            P("section", "mp", None),
        ),
        out_specs=(
            P("section", None, "dp", "mp", None),
            P("section", None, "dp", "mp", None),
            P("section", None),
            P("section", None, None, "mp"),
            P("section", None, None),
            P("section", None, "mp"),
            P("section", None, "mp"),
            P("section", None, None),
            P("section", "mp"),
            P("section", "mp"),
            P("section", "mp"),
            P("section", "mp"),
            P("section", "mp", None),
        ),
        check_vma=False,
    )
```

```python
import functools
import jax
import jax.numpy as jnp
from jax import lax
from jax.experimental import pallas as pl
from jax.experimental.pallas import tpu as pltpu
from jax.sharding import PartitionSpec as P

epsilon = 1e-05
f32 = jnp.float32
bf16 = jnp.bfloat16
highest = lax.Precision.HIGHEST
BLOCK = 256
HALO = 8
LOG2E = 1.4426950408889634


def mm(a, b, contract, precision=None):
    return lax.dot_general(a, b, (contract, ((), ())), preferred_element_type=f32, precision=precision)


NN = ((1,), (0,))
NT = ((1,), (1,))
TN = ((0,), (0,))


def sigmoid(v):
    return 0.5 * jnp.tanh(0.5 * v) + 0.5


def step_of(z):
    e = jnp.exp(-jnp.abs(z))
    u = 1.0 + e
    d = u - 1.0
    tail = jnp.where(d == 0.0, e, jnp.log(u) * (e / jnp.where(d == 0.0, 1.0, d)))
    return jnp.maximum(z, 0.0) + tail


def triangle(inclusive, upper=False):
    r = lax.broadcasted_iota(jnp.int32, (BLOCK, BLOCK), 0)
    c = lax.broadcasted_iota(jnp.int32, (BLOCK, BLOCK), 1)
    if upper:
        r, c = c, r
    return (r >= c) if inclusive else (r > c)


def pad_lanes(v, to=128):
    return jnp.concatenate([v, jnp.zeros((v.shape[0], to - v.shape[1]), v.dtype)], axis=1)


def low_half(shape):
    return lax.broadcasted_iota(jnp.int32, shape, 1) < 64


def pair_of(cols, p):
    rows = cols.shape[0]
    lo = low_half((rows, 128))
    return jnp.where(lo, cols[:, 2 * p : 2 * p + 1], cols[:, 2 * p + 1 : 2 * p + 2])


def block_setup(step_pre, bias, decay, heads):
    z = step_pre + bias
    step = step_of(z)
    rate = jnp.exp(decay)
    dec = pad_lanes(step * rate)
    tri = triangle(True).astype(f32)
    ld = -mm(tri, dec, NN, highest)[:, :heads]
    return z, step, rate, ld


def fwd_kernel(sizes, pre, taps, heads3, mixed, gated_out, sq, states, ext, carry, scr):
    inner, state, heads = sizes
    k = pl.program_id(0)
    nst = state // 2
    pairs = heads // 2
    a_state, a_step = 2 * inner, 2 * inner + state

    @pl.when(k == 0)
    def _():
        ext[0:HALO, :] = jnp.zeros((HALO, inner + state), f32)
        carry[...] = jnp.zeros_like(carry)

    ext[HALO:, :] = pre[:, inner:a_step]

    def act(lo, width):
        c = taps[0:1, lo : lo + width] * ext[HALO - 3 : HALO - 3 + BLOCK, lo : lo + width]
        for j in range(1, 4):
            c = c + taps[j : j + 1, lo : lo + width] * ext[HALO - 3 + j : HALO - 3 + j + BLOCK, lo : lo + width]
        return (c * sigmoid(c)).astype(bf16)

    b = act(inner, nst)
    c = act(inner + nst, nst)
    z, step, rate, ld = block_setup(pre[:, a_step : a_step + heads], heads3[0:1, :heads], heads3[1:2, :heads], heads)
    ld2 = ld * LOG2E
    rrow = jnp.transpose(pad_lanes(jnp.log2(step) - ld2))
    eld = jnp.exp2(ld2)
    last = ld2[BLOCK - 1 : BLOCK, :]
    tail = jnp.exp2(last - ld2) * step
    scr[...] = jnp.where(triangle(True), mm(c, b, NT), 0.0)
    squares = jnp.zeros((BLOCK, 1), f32)
    half = BLOCK // 2
    for p in range(pairs):
        lanes = slice(128 * p, 128 * p + 128)
        x = act(128 * p, 128)
        xf = x.astype(f32)
        lo = low_half((BLOCK, 128))
        xs = [jnp.where(lo, x, jnp.zeros_like(x)), jnp.where(lo, jnp.zeros_like(x), x)]
        tops, bottoms = [], []
        for i in range(2):
            h = 2 * p + i
            top = jnp.exp2(jnp.minimum(ld2[:half, h : h + 1] + rrow[h : h + 1, :half], 40.0)) * scr[:half, :half]
            tops.append(mm(top.astype(bf16), xs[i][:half], NN))
            bot = jnp.exp2(jnp.minimum(ld2[half:, h : h + 1] + rrow[h : h + 1, :], 40.0)) * scr[half:, :]
            bottoms.append(mm(bot.astype(bf16), xs[i], NN))
        within = jnp.concatenate([tops[0] + tops[1], bottoms[0] + bottoms[1]], axis=0)
        s_in = carry[:, lanes]
        e_pair = pair_of(eld, p)
        cross = mm(c, s_in.astype(bf16), NN) * e_pair
        y = within + cross + pair_of(heads3[2:3, :heads], p) * xf
        mixed[:, lanes] = y
        g = pre[:, lanes]
        gated = y * (g * sigmoid(g))
        squares = squares + jnp.sum(gated * gated, axis=1, keepdims=True)
        gated_out[:, lanes] = gated
        s_out = e_pair[BLOCK - 1 :, :] * s_in + mm(b, (xf * pair_of(tail, p)).astype(bf16), TN)
        carry[:, lanes] = s_out
        states[0, :, lanes] = s_out
    sq[0] = jnp.transpose(pad_lanes(squares))[0:1, :]
    ext[0:HALO, :] = ext[BLOCK : BLOCK + HALO, :]


def mix_forward(pre, taps, heads3, inner, state, heads):
    rows = pre.shape[0]
    blocks = rows // BLOCK
    width = pre.shape[1]
    nst = state // 2
    return pl.pallas_call(
        functools.partial(fwd_kernel, (inner, state, heads)),
        grid=(blocks,),
        in_specs=[
            pl.BlockSpec((BLOCK, width), lambda k: (k, 0)),
            pl.BlockSpec((4, inner + state), lambda k: (0, 0)),
            pl.BlockSpec((3, heads), lambda k: (0, 0)),
        ],
        out_specs=[
            pl.BlockSpec((BLOCK, inner), lambda k: (k, 0)),
            pl.BlockSpec((BLOCK, inner), lambda k: (k, 0)),
            pl.BlockSpec((1, 1, BLOCK), lambda k: (k, 0, 0)),
            pl.BlockSpec((1, nst, inner), lambda k: (k, 0, 0)),
        ],
        out_shape=[
            jax.ShapeDtypeStruct((rows, inner), f32),
            jax.ShapeDtypeStruct((rows, inner), f32),
            jax.ShapeDtypeStruct((blocks, 1, BLOCK), f32),
            jax.ShapeDtypeStruct((blocks, nst, inner), f32),
        ],
        scratch_shapes=[
            pltpu.VMEM((BLOCK + HALO, inner + state), f32),
            pltpu.VMEM((nst, inner), f32),
            pltpu.VMEM((BLOCK, BLOCK), f32),
        ],
        name="mix_forward",
    )(pre, taps, heads3)


def gate_kernel(pre, mixed, ngrad, rows2, gain, normed, dgate, dy, g_gain):
    @pl.when(pl.program_id(0) == 0)
    def _():
        g_gain[...] = jnp.zeros_like(g_gain)

    inv = rows2[:, 0:1]
    pull = rows2[:, 1:2]
    for lo in range(0, mixed.shape[1], 128):
        lanes = slice(lo, lo + 128)
        g = pre[:, lanes]
        sg = sigmoid(g)
        silu = g * sg
        y = mixed[:, lanes]
        gated = y * silu
        ng = ngrad[:, lanes]
        gn = gain[:, lanes]
        gi = gated * inv
        normed[:, lanes] = (gi * gn).astype(bf16)
        g_gain[:, lanes] += jnp.sum(ng * gi, axis=0, keepdims=True)
        gg = inv * (ng * gn) - gated * pull
        dgate[:, lanes] = (gg * y * (sg * (1.0 + g * (1.0 - sg)))).astype(bf16)
        dy[:, lanes] = gg * silu


def gate_backward(pre, mixed, ngrad, rows2, gain, inner):
    rows = pre.shape[0]
    block = pl.BlockSpec((BLOCK, inner), lambda k: (k, 0))
    return pl.pallas_call(
        gate_kernel,
        grid=(rows // BLOCK,),
        in_specs=[block, block, block, pl.BlockSpec((BLOCK, 2), lambda k: (k, 0)), pl.BlockSpec((1, inner), lambda k: (0, 0))],
        out_specs=[block, block, block, pl.BlockSpec((1, inner), lambda k: (0, 0))],
        out_shape=[
            jax.ShapeDtypeStruct((rows, inner), bf16),
            jax.ShapeDtypeStruct((rows, inner), bf16),
            jax.ShapeDtypeStruct((rows, inner), f32),
            jax.ShapeDtypeStruct((1, inner), f32),
        ],
        name="gate_backward",
    )(pre, mixed, ngrad, rows2, gain)


def bwd_kernel(sizes, pre, halo, dgate, dyin, s_in_ref, taps, heads3,
               own, g_taps, g_heads, ext, dext, carry, acc, scr, dyb, xb, cold, rowd, xw):
    inner, state, heads = sizes
    step_id = pl.program_id(0)
    blocks = pl.num_programs(0)
    k = blocks - 1 - step_id
    nst = state // 2
    pairs = heads // 2
    a_state, a_step = 2 * inner, 2 * inner + state

    @pl.when(step_id == 0)
    def _():
        dext[BLOCK:, :] = jnp.zeros((HALO, inner + state), f32)
        carry[...] = jnp.zeros_like(carry)
        g_taps[...] = jnp.zeros_like(g_taps)
        g_heads[...] = jnp.zeros_like(g_heads)

    own[:, :inner] = dgate[...]
    ext[HALO:, :] = pre[:, inner:a_step]
    ext[0:HALO, :] = jnp.where(k == 0, 0.0, halo[:, inner:a_step])

    def conv(lo, width):
        c = taps[0:1, lo : lo + width] * ext[HALO - 3 : HALO - 3 + BLOCK, lo : lo + width]
        for j in range(1, 4):
            c = c + taps[j : j + 1, lo : lo + width] * ext[HALO - 3 + j : HALO - 3 + j + BLOCK, lo : lo + width]
        return c

    def dsilu(v):
        s = sigmoid(v)
        return s * (1.0 + v * (1.0 - s))

    cb = conv(inner, nst)
    cc = conv(inner + nst, nst)
    b = (cb * sigmoid(cb)).astype(bf16)
    c = (cc * sigmoid(cc)).astype(bf16)
    z, step, rate, ld = block_setup(pre[:, a_step : a_step + heads], heads3[0:1, :heads], heads3[1:2, :heads], heads)
    ld2 = ld * LOG2E
    ldrow = jnp.transpose(pad_lanes(ld2))
    rcol = jnp.log2(step) - ld2
    eld = jnp.exp2(ld2)
    tail = jnp.exp2(ld2[BLOCK - 1 : BLOCK, :] - ld2) * step
    scr[...] = jnp.where(triangle(True, upper=True), mm(b, c, NT), 0.0)
    acc[...] = jnp.zeros_like(acc)
    half = BLOCK // 2
    d_b = jnp.zeros((BLOCK, nst), f32)
    d_c = jnp.zeros((BLOCK, nst), f32)
    head_lane = lax.broadcasted_iota(jnp.int32, (1, 128), 1)
    cold[...] = jnp.zeros_like(cold)
    xw[...] = jnp.zeros_like(xw)
    carried = jnp.zeros((1, 128), f32)
    skips = jnp.zeros((1, 128), f32)
    for p in range(pairs):
        lanes = slice(128 * p, 128 * p + 128)
        lo = low_half((BLOCK, 128))
        lo1 = low_half((1, 128))
        dy = dyin[:, lanes]
        cx = conv(128 * p, 128)
        sx = sigmoid(cx)
        x = (cx * sx).astype(bf16)
        xf = x.astype(f32)
        dyh = dy.astype(bf16)
        zero = jnp.zeros_like(x)
        xs = [jnp.where(lo, x, zero), jnp.where(lo, zero, x)]
        dys = [jnp.where(lo, dyh, zero), jnp.where(lo, zero, dyh)]
        tops, bottoms = [], []
        for i in range(2):
            h = 2 * p + i
            w_top = jnp.exp2(jnp.minimum(ldrow[h : h + 1, :] + rcol[:half, h : h + 1], 40.0))
            s_top = scr[:half, :]
            m_top = w_top * s_top
            tops.append(mm(m_top.astype(bf16), dys[i], NN))
            gm = mm(xs[i][:half], dyh, NT) * w_top
            acc[:half, :] += gm
            e_top = gm * s_top
            w_bot = jnp.exp2(jnp.minimum(ldrow[h : h + 1, half:] + rcol[half:, h : h + 1], 40.0))
            s_bot = scr[half:, half:]
            m_bot = w_bot * s_bot
            bottoms.append(mm(m_bot.astype(bf16), dys[i][half:], NN))
            gm = mm(xs[i][half:], dyh[half:], NT) * w_bot
            acc[half:, half:] += gm
            e_bot = gm * s_bot
            cold[:half, h : h + 1] = jnp.sum(e_top, axis=1, keepdims=True)
            cold[half:, h : h + 1] = jnp.sum(e_bot, axis=1, keepdims=True)
            top_row = jnp.sum(e_top, axis=0, keepdims=True)
            rowd[h : h + 1, :half] = top_row[:, :half]
            rowd[h : h + 1, half:] = top_row[:, half:] + jnp.sum(e_bot, axis=0, keepdims=True)
        dxm = jnp.concatenate([tops[0] + tops[1], bottoms[0] + bottoms[1]], axis=0)
        ds = carry[:, lanes]
        dsh = ds.astype(bf16)
        s_in = jnp.where(k == 0, 0.0, s_in_ref[0, :, lanes])
        s_h = s_in.astype(bf16)
        e_pair = pair_of(eld, p)
        t_pair = pair_of(tail, p)
        dye = (dy * e_pair).astype(bf16)
        cross = mm(c, s_h, NN) * e_pair * dy
        w = mm(b, dsh, NN) * t_pair
        wx = w * xf
        for i in range(2):
            h = 2 * p + i
            keep = lo if i == 0 else jnp.logical_not(lo)
            xw[:, h : h + 1] = jnp.sum(jnp.where(keep, wx, 0.0), axis=1, keepdims=True)
            xw[:, 64 + h : 65 + h] = jnp.sum(jnp.where(keep, cross, 0.0), axis=1, keepdims=True)
        d_c = d_c + mm(dye, s_h, NT)
        d_b = d_b + mm((xf * t_pair).astype(bf16), dsh, NT)
        skip_pair = pair_of(heads3[2:3, :heads], p)
        dx = dxm + skip_pair * dy + w
        dskip = jnp.sum(dy * xf, axis=0, keepdims=True)
        dstate = jnp.sum(ds * s_in, axis=0, keepdims=True) * e_pair[BLOCK - 1 :, :]
        for i in range(2):
            h = 2 * p + i
            keep = lo1 if i == 0 else jnp.logical_not(lo1)
            skips = jnp.where(head_lane == h, jnp.sum(jnp.where(keep, dskip, 0.0), axis=1, keepdims=True), skips)
            carried = jnp.where(head_lane == h, jnp.sum(jnp.where(keep, dstate, 0.0), axis=1, keepdims=True), carried)
        carry[:, lanes] = e_pair[BLOCK - 1 :, :] * ds + mm(c, dye, TN)
        dext[:BLOCK, lanes] = dx * (sx * (1.0 + cx * (1.0 - sx)))
    ah = jnp.where(triangle(True, upper=True), acc[...], 0.0).astype(bf16)
    d_b = d_b + mm(ah, c, NN)
    d_c = d_c + mm(ah, b, TN)
    dext[:BLOCK, inner : inner + nst] = d_b * dsilu(cb)
    dext[:BLOCK, inner + nst :] = d_c * dsilu(cc)
    colsum = cold[...]
    rowsum = jnp.transpose(jnp.concatenate([rowd[...], jnp.zeros((128 - heads, BLOCK), f32)], axis=0))
    xwv = xw[...]
    crossv = pltpu.roll(xwv, 64, 1)
    lane = lax.broadcasted_iota(jnp.int32, (BLOCK, 128), 1)
    tailv = jnp.where(lane < heads, xwv, 0.0)
    crossv = jnp.where(lane < heads, crossv, 0.0)
    upper = triangle(True, upper=True).astype(f32)
    strict = triangle(False).astype(f32)
    from_q = mm(upper, rowsum - colsum + crossv, NN, highest) + mm(strict, tailv, NN, highest) + carried
    ddec = -from_q[:, :heads]
    q = (colsum + tailv)[:, :heads]
    sz = sigmoid(z)
    ratio = jnp.where(step > 1e-30, sz / jnp.where(step > 1e-30, step, 1.0), 1.0)
    dz = q * ratio + rate * ddec * sz
    own[:, a_step:] = pad_lanes(dz, own.shape[1] - a_step).astype(bf16)
    g_heads[0:1, :heads] += jnp.sum(dz, axis=0, keepdims=True)
    g_heads[1:2, :heads] += rate * jnp.sum(step * ddec, axis=0, keepdims=True)
    g_heads[2:3, :] += skips
    for at in range(0, inner + state, 256):
        lanes = slice(at, at + 256)
        dpre = taps[3:4, lanes] * dext[0:BLOCK, lanes]
        for j in range(3):
            dpre = dpre + taps[j : j + 1, lanes] * dext[3 - j : 3 - j + BLOCK, lanes]
        own[:, inner + at : inner + at + 256] = dpre.astype(bf16)
        d = dext[0:BLOCK, lanes]
        for j in range(4):
            g_taps[j : j + 1, lanes] += jnp.sum(d * ext[HALO - 3 + j : HALO - 3 + j + BLOCK, lanes], axis=0, keepdims=True)
    dext[BLOCK:, :] = dext[0:HALO, :]


def mix_backward(pre, dgate, dy, states, taps, heads3, inner, state, heads):
    rows = pre.shape[0]
    blocks = rows // BLOCK
    width = pre.shape[1]
    nst = state // 2
    last = blocks - 1
    per = BLOCK // HALO
    return pl.pallas_call(
        functools.partial(bwd_kernel, (inner, state, heads)),
        grid=(blocks,),
        in_specs=[
            pl.BlockSpec((BLOCK, width), lambda k: (last - k, 0)),
            pl.BlockSpec((HALO, width), lambda k: (jnp.maximum((last - k) * per - 1, 0), 0)),
            pl.BlockSpec((BLOCK, inner), lambda k: (last - k, 0)),
            pl.BlockSpec((BLOCK, inner), lambda k: (last - k, 0)),
            pl.BlockSpec((1, nst, inner), lambda k: (jnp.maximum(last - k - 1, 0), 0, 0)),
            pl.BlockSpec((4, inner + state), lambda k: (0, 0)),
            pl.BlockSpec((3, heads), lambda k: (0, 0)),
        ],
        out_specs=[
            pl.BlockSpec((BLOCK, width), lambda k: (last - k, 0)),
            pl.BlockSpec((4, inner + state), lambda k: (0, 0)),
            pl.BlockSpec((8, 128), lambda k: (0, 0)),
        ],
        out_shape=[
            jax.ShapeDtypeStruct((rows, width), bf16),
            jax.ShapeDtypeStruct((4, inner + state), f32),
            jax.ShapeDtypeStruct((8, 128), f32),
        ],
        scratch_shapes=[
            pltpu.VMEM((BLOCK + HALO, inner + state), f32),
            pltpu.VMEM((BLOCK + HALO, inner + state), f32),
            pltpu.VMEM((nst, inner), f32),
            pltpu.VMEM((BLOCK, BLOCK), f32),
            pltpu.VMEM((BLOCK, BLOCK), f32),
            pltpu.VMEM((8, 128), f32),
            pltpu.VMEM((8, 128), f32),
            pltpu.VMEM((BLOCK, 128), f32),
            pltpu.VMEM((heads, BLOCK), f32),
            pltpu.VMEM((BLOCK, 128), f32),
        ],
        name="mix_backward",
    )(pre, pre, dgate, dy, states, taps, heads3)


MESH = pl.DeviceIdType.MESH
ANY = pl.BlockSpec(memory_space=pl.ANY)
VM = pl.BlockSpec(memory_space=pltpu.VMEM)


def at(section=None, dp=None, mp=None):
    return (
        lax.axis_index("section") if section is None else section,
        lax.axis_index("dp") if dp is None else dp,
        lax.axis_index("mp") if mp is None else mp,
    )


def send(src, dst, send_sem, recv_sem, where):
    return pltpu.make_async_remote_copy(
        src_ref=src, dst_ref=dst, send_sem=send_sem, recv_sem=recv_sem, device_id=where, device_id_type=MESH
    )


def greet(peers):
    barrier = pltpu.get_barrier_semaphore()
    for peer in peers:
        pl.semaphore_signal(barrier, inc=1, device_id=peer, device_id_type=MESH)
    pl.semaphore_wait(barrier, len(peers))


def others(axis, count):
    me = lax.axis_index(axis)
    return [lax.rem(me + i, count) for i in range(1, count)]


def reduce_kernel(counts, layout, chunk, *refs):
    items = len(layout)
    sections, dps, mps = counts
    xs, ts, os = refs[:items], refs[items : 2 * items], refs[2 * items : 3 * items]
    ls, r1s, r2s, r3s, qs = (refs[(3 + i) * items : (4 + i) * items] for i in range(5))
    rs, load_sem, s1, d1, s2, d2, s3, d3, sm, dm, s4, d4, out_sem = refs[8 * items :]
    section, d, m = lax.axis_index("section"), lax.axis_index("dp"), lax.axis_index("mp")
    core = d + 1 - 2 * lax.rem(d, 2)
    far = lax.rem(d + 2, 4)
    core_far = lax.rem(core + 2, 4)
    to_core, to_far, to_section = at(dp=core), at(dp=far), at(section=1 - section)
    mp_peers = others("mp", mps)
    greet([to_core, to_far, to_section] + [at(mp=j) for j in mp_peers])

    class Unit:
        pass

    units = []
    for item, (ready, t_cols, state) in enumerate(layout):
        quarter = os[item].shape[0] // 4
        step = min(chunk, quarter)
        for base in range(0, quarter, step):
            u = Unit()
            u.n, u.item, u.ready, u.state, u.quarter, u.base, u.step = len(units), item, ready, state, quarter, base, step
            u.x, u.o, u.l, u.r1, u.r2, u.r3, u.q = xs[item], os[item], ls[item], r1s[item], r2s[item], r3s[item], qs[item]
            u.rows = pl.ds(base, step)
            u.t = ts[item].at[u.rows, t_cols]
            units.append(u)

    def of_quarter(u, index):
        return pl.ds(pl.multiple_of(index * u.quarter + u.base, 16), u.step)

    for u in units:
        u.early = send(u.t, u.r3.at[u.rows], s3.at[u.n], d3.at[u.n], to_section)
        if u.ready:
            u.third = send(u.x.at[u.rows], u.r3.at[u.rows], s3.at[u.n], d3.at[u.n], to_section)
        else:
            u.third = send(u.l.at[0, u.rows], u.r3.at[u.rows], s3.at[u.n], d3.at[u.n], to_section)

        @pl.when(section == 0)
        def _():
            u.early.start()

        if u.ready:

            @pl.when(section == 1)
            def _():
                u.third.start()

            continue
        u.first, u.loads = {}, {}
        for i, own, theirs in ((1, far, core_far), (0, d, core)):
            u.first[i] = send(u.x.at[of_quarter(u, theirs)], u.r1.at[i, u.rows], s1.at[u.n, i], d1.at[u.n, i], to_core)
            u.first[i].start()
            u.loads[i] = pltpu.make_async_copy(u.x.at[of_quarter(u, own)], u.l.at[i, u.rows], load_sem.at[u.n, i])
            u.loads[i].start()

    outs = []

    def stage2(u):
        if u.ready:
            return
        u.first[1].wait_recv()
        u.loads[1].wait()
        u.l[1, u.rows] = (u.l[1, u.rows].astype(f32) + u.r1[1, u.rows].astype(f32)).astype(bf16)
        u.second = send(u.l.at[1, u.rows], u.r2.at[u.rows], s2.at[u.n], d2.at[u.n], to_far)
        u.second.start()

    def stage3(u):
        if u.ready:
            return
        u.first[0].wait_recv()
        u.loads[0].wait()
        u.second.wait_recv()

        @pl.when(section == 1)
        def _():
            u.l[0, u.rows] = (
                u.l[0, u.rows].astype(f32) + u.r1[0, u.rows].astype(f32) + u.r2[u.rows].astype(f32)
            ).astype(bf16)
            u.third.start()

    def stage4(u):
        u.third.wait_recv()

        @pl.when(section == 0)
        def _():
            if u.ready:
                u.q[0, u.rows] = (u.x[u.rows].astype(f32) + u.r3[u.rows].astype(f32)).astype(bf16)
            else:
                u.q[0, u.rows] = (
                    u.l[0, u.rows].astype(f32)
                    + u.r1[0, u.rows].astype(f32)
                    + u.r2[u.rows].astype(f32)
                    + u.r3[u.rows].astype(f32)
                ).astype(bf16)

        @pl.when(section == 1)
        def _():
            u.q[0, u.rows] = (u.t[...].astype(f32) + u.r3[u.rows].astype(f32)).astype(bf16)

        u.mixes = []
        if u.state is not None:
            rs[m, u.rows] = u.q[0, u.rows, u.state]
            for i, j in enumerate(mp_peers):
                c = send(rs.at[m, u.rows], rs.at[m, u.rows], sm.at[u.n, i], dm.at[u.n, i], at(mp=j))
                c.start()
                u.mixes.append(c)

    def output(u, slot, index):
        c = pltpu.make_async_copy(u.q.at[slot, u.rows], u.o.at[of_quarter(u, index)], out_sem.at[u.n, slot])
        c.start()
        outs.append(c)

    def stage5(u):
        if u.state is not None:
            for c in u.mixes:
                c.wait_recv()
            total = rs[0, u.rows].astype(f32)
            for j in range(1, mps):
                total = total + rs[j, u.rows].astype(f32)
            u.q[0, u.rows, u.state] = total.astype(bf16)
        u.fourth = [
            send(u.q.at[0, u.rows], u.q.at[1, u.rows], s4.at[u.n, 0], d4.at[u.n, 0], to_far),
            send(u.q.at[0, u.rows], u.q.at[2, u.rows], s4.at[u.n, 1], d4.at[u.n, 1], to_core),
            send(u.q.at[1, u.rows], u.q.at[3, u.rows], s4.at[u.n, 2], d4.at[u.n, 2], to_core),
        ]
        u.fourth[0].start()
        u.fourth[1].start()
        output(u, 0, d)

    def stage6(u):
        u.fourth[0].wait_recv()
        u.fourth[2].start()
        output(u, 1, far)

    def stage7(u):
        u.fourth[1].wait_recv()
        output(u, 2, core)
        u.fourth[2].wait_recv()
        output(u, 3, core_far)

    stages = (stage2, stage3, stage4, stage5, stage6, stage7)
    for tick in range(len(units) + len(stages) - 1):
        for lag, stage in enumerate(stages):
            if 0 <= tick - lag < len(units):
                stage(units[tick - lag])
    for u in units:
        if not u.ready:
            u.first[0].wait_send()
            u.first[1].wait_send()
            u.second.wait_send()
        u.third.wait_send()
        for c in u.fourth + u.mixes:
            c.wait_send()
    for c in outs:
        c.wait()


def reduce_all(items, counts):
    chunk = 128
    mps = counts[2]
    dma = pltpu.SemaphoreType.DMA
    layout, sizes, n, ua = [], [], 0, 1
    state_rows, state_width = 8, 128
    for x, t, column, ready, state in items:
        quarter = x.shape[0] if ready else x.shape[0] // 4
        width = x.shape[1]
        layout.append((ready, pl.ds(column, width), None if state is None else pl.ds(*state)))
        sizes.append((quarter, width, ready))
        n += max(1, quarter // chunk)
        if state is not None:
            state_rows, state_width = quarter, state[1]
    tiny = (2, 16, 128)
    scratch = [pltpu.VMEM(tiny if ready else (2, q, w), bf16) for q, w, ready in sizes] * 2
    scratch += [pltpu.VMEM(tiny[1:] if ready else (q, w), bf16) for q, w, ready in sizes]
    scratch += [pltpu.VMEM((q, w), bf16) for q, w, ready in sizes]
    scratch += [pltpu.VMEM((4, q, w), bf16) for q, w, ready in sizes]
    return pl.pallas_call(
        functools.partial(reduce_kernel, counts, tuple(layout), chunk),
        in_specs=[VM if ready else ANY for q, w, ready in sizes] + [VM] * len(items),
        out_specs=[ANY] * len(items),
        out_shape=[jax.ShapeDtypeStruct((4 * q, w), bf16) for q, w, ready in sizes],
        scratch_shapes=scratch
        + [
            pltpu.VMEM((mps, state_rows, state_width), bf16),
            dma((n, 2)),
            dma((n, 2)),
            dma((n, 2)),
            dma((n,)),
            dma((n,)),
            dma((n,)),
            dma((n,)),
            dma((n, max(1, mps - 1))),
            dma((n, max(1, mps - 1))),
            dma((n, 3)),
            dma((n, 3)),
            dma((n, 4)),
        ],
        compiler_params=pltpu.CompilerParams(collective_id=1, has_side_effects=True),
        cost_estimate=pl.CostEstimate(flops=10**7, bytes_accessed=3 * 10**8, transcendentals=0),
        name="reduce_all",
    )(*[i[0] for i in items], *[i[1] for i in items])


def small_kernel(counts, a, b, oa, ob, ba, bb, ca, cb, zb, sems, recvs):
    sections, dps, mps = counts
    section, d, m = lax.axis_index("section"), lax.axis_index("dp"), lax.axis_index("mp")
    groups = [
        [at(section=j) for j in others("section", sections)],
        [at(dp=j) for j in others("dp", dps)],
        [at(mp=j) for j in others("mp", mps)],
    ]
    greet(groups[0] + groups[1] + groups[2])
    at_sem = 0

    def exchange(buffers, mine, peers):
        nonlocal at_sem
        copies = []
        for peer in peers:
            for buffer in buffers:
                c = send(buffer.at[mine], buffer.at[mine], sems.at[at_sem], recvs.at[at_sem], peer)
                c.start()
                copies.append(c)
                at_sem += 1
        for c in copies:
            c.wait()

    def total(buffer, count):
        v = buffer[0]
        for j in range(1, count):
            v = v + buffer[j]
        return v

    ba[section] = a[...]
    bb[section] = b[...]
    exchange([ba, bb], section, groups[0])
    ca[d] = total(ba, sections)
    cb[d] = total(bb, sections)
    exchange([ca, cb], d, groups[1])
    oa[...] = total(ca, dps)
    zb[m] = total(cb, dps)
    exchange([zb], m, groups[2])
    ob[...] = total(zb, mps)


def small_reduce(a, b, counts):
    sections, dps, mps = counts
    n = 2 * (sections - 1) + 2 * (dps - 1) + (mps - 1)
    dma = pltpu.SemaphoreType.DMA
    return pl.pallas_call(
        functools.partial(small_kernel, counts),
        in_specs=[VM, VM],
        out_specs=[VM, VM],
        out_shape=[jax.ShapeDtypeStruct(a.shape, f32), jax.ShapeDtypeStruct(b.shape, f32)],
        scratch_shapes=[
            pltpu.VMEM((sections,) + a.shape, f32),
            pltpu.VMEM((sections,) + b.shape, f32),
            pltpu.VMEM((dps,) + a.shape, f32),
            pltpu.VMEM((dps,) + b.shape, f32),
            pltpu.VMEM((mps,) + b.shape, f32),
            dma((n,)),
            dma((n,)),
        ],
        compiler_params=pltpu.CompilerParams(collective_id=2, has_side_effects=True),
        cost_estimate=pl.CostEstimate(flops=10**6, bytes_accessed=3 * 10**7, transcendentals=0),
        name="small_reduce",
    )(a, b)


def format_kernel(inner, state, heads, gate, rest, g_in, g_state, g_step):
    g_in[:, 0, :] = gate[...].astype(f32)
    g_in[:, 1, :] = rest[:, :inner].astype(f32)
    g_state[...] = rest[:, inner : inner + state].astype(f32)
    g_step[...] = rest[:, inner + state : inner + state + heads].astype(f32)


def format_grads(gate, rest, inner, state, heads):
    rows = gate.shape[0]
    step = 256
    return pl.pallas_call(
        functools.partial(format_kernel, inner, state, heads),
        grid=(rows // step,),
        in_specs=[pl.BlockSpec((step, v.shape[1]), lambda i: (i, 0)) for v in (gate, rest)],
        out_specs=[
            pl.BlockSpec((step, 2, inner), lambda i: (i, 0, 0)),
            pl.BlockSpec((step, state), lambda i: (i, 0)),
            pl.BlockSpec((step, heads), lambda i: (i, 0)),
        ],
        out_shape=[
            jax.ShapeDtypeStruct((rows, 2, inner), f32),
            jax.ShapeDtypeStruct((rows, state), f32),
            jax.ShapeDtypeStruct((rows, heads), f32),
        ],
        cost_estimate=pl.CostEstimate(flops=10**6, bytes_accessed=3 * 10**7, transcendentals=0),
        name="format_grads",
    )(gate, rest)


def pick(condition, one, other):
    return jnp.where(condition, one, other)


def load_weight(layer, w, w_other, wv, w_sem):
    load = pltpu.make_async_copy(w, wv, w_sem)
    if layer is None:
        load.start()
        return load
    section = lax.axis_index("section")

    @pl.when(section == layer)
    def _():
        load.start()

    @pl.when(section != layer)
    def _():
        pltpu.make_async_copy(w_other, wv, w_sem).start()

    return load


def line_barrier(n, with_section=False):
    m = lax.axis_index("mp")
    barrier = pltpu.get_barrier_semaphore()
    if with_section:
        pl.semaphore_signal(barrier, inc=1, device_id=at(section=1 - lax.axis_index("section")), device_id_type=MESH)

    @pl.when(m > 0)
    def _():
        pl.semaphore_signal(barrier, inc=1, device_id=at(mp=m - 1), device_id_type=MESH)

    @pl.when(m < n - 1)
    def _():
        pl.semaphore_signal(barrier, inc=1, device_id=at(mp=m + 1), device_id_type=MESH)

    pl.semaphore_wait(barrier, pick(m > 0, 1, 0) + pick(m < n - 1, 1, 0) + int(with_section))


def arrival(p, m, n):
    both = jnp.minimum(m, n - 1 - m)
    inside = p <= 2 * both
    t = pick(inside, (p + 1) // 2, p - both)
    left = pick(inside, lax.rem(p, 2) == 1, m > n - 1 - m)
    return pick(left, m - t, m + t)


def gather_kernel(n, transposed, tile, layer, swaps, *refs):
    x, side, w, w_other = refs[:4]
    refs = refs[4:]
    if swaps:
        of_first, of_second, theirs = refs[0], refs[1], refs[5]
        refs = refs[2:5] + refs[6:]
    gathered, sides, product, buf, sbuf, wv, stage = refs[:7]
    own_sem, fwd_sem, recv_sem, sown_sem, sfwd_sem, srecv_sem, w_sem, g_sem, p_sem = refs[7:16]
    m = lax.axis_index("mp")
    rows = x.shape[0]
    load = load_weight(layer, w, w_other, wv, w_sem)
    line_barrier(n, swaps)
    has_left, has_right = m > 0, m < n - 1
    if swaps:
        section = lax.axis_index("section")
        y_send, y_recv = refs[16:]

        def swap_move(source):
            return send(source, theirs, y_send, y_recv, at(section=1 - section))

        @pl.when(section == 0)
        def _():
            swap_move(of_first).start()

        @pl.when(section == 1)
        def _():
            swap_move(of_second).start()


    parts = own_sem.shape[1]
    cut = [pl.ds(i * (rows // parts), rows // parts) for i in range(parts)]

    def small(shard, ssrc, ssem, to):
        return send(ssrc, sbuf.at[shard], ssem, srecv_sem.at[shard], at(mp=to))

    def own_moves(way, to):
        return [send(x.at[c], buf.at[m, c], own_sem.at[way, i], recv_sem.at[m, i], at(mp=to)) for i, c in enumerate(cut)] + [
            small(m, side, sown_sem.at[way], to)
        ]

    def own_left():
        return own_moves(0, m - 1)

    def own_right():
        return own_moves(1, m + 1)

    @pl.when(has_left)
    def _():
        for c in own_left():
            c.start()

    @pl.when(has_right)
    def _():
        for c in own_right():
            c.start()

    buf[m] = x[...]
    sbuf[m] = side[...]
    load.wait()

    def toward(shard):
        return pick(shard < m, jnp.minimum(m + 1, n - 1), jnp.maximum(m - 1, 0))

    def forward_part(shard, i):
        c = cut[i]
        return send(buf.at[shard, c], buf.at[shard, c], fwd_sem.at[shard, i], recv_sem.at[shard, i], at(mp=toward(shard)))

    def forward_small(shard):
        return small(shard, sbuf.at[shard], sfwd_sem.at[shard], toward(shard))

    def forward(shard):
        return [forward_part(shard, i) for i in range(parts)] + [forward_small(shard)]

    def passes_on(shard):
        return pick(shard < m, jnp.logical_and(has_right, shard >= 0), jnp.logical_and(has_left, shard > m))

    def out_copy(shard):
        return pltpu.make_async_copy(buf.at[shard], gathered.at[pl.ds(pl.multiple_of(shard * rows, rows), rows)], g_sem.at[shard])

    def put(shard, slot):
        return pltpu.make_async_copy(stage.at[slot], product.at[pl.ds(pl.multiple_of(shard * rows, rows), rows)], p_sem.at[slot])

    def body(p, _):
        shard = arrival(p, m, n)

        @pl.when(p > 0)
        def _():
            for i in range(parts):
                forward_part(shard, i).wait_recv()

                @pl.when(passes_on(shard))
                def _():
                    forward_part(shard, i).start()

            forward_small(shard).wait_recv()

            @pl.when(passes_on(shard))
            def _():
                forward_small(shard).start()

        out_copy(shard).start()
        slot = lax.rem(p, 2)

        @pl.when(p > 1)
        def _():
            put(shard, slot).wait()

        def columns(cols):
            if transposed:
                stage[slot, :, cols] = mm(buf[shard], wv[cols, :], NT)
            else:
                stage[slot, :, cols] = mm(buf[shard], wv[:, cols], NN)

        def column(i, _):
            columns(pl.ds(pl.multiple_of(i * tile, tile), tile))
            return 0

        width = product.shape[1]
        lax.fori_loop(0, width // tile, column, 0)
        if width % tile:
            columns(pl.ds(width - width % tile, width % tile))
        put(shard, slot).start()
        return 0

    lax.fori_loop(0, n, body, 0)

    @pl.when(has_left)
    def _():
        for c in own_left():
            c.wait_send()

    @pl.when(has_right)
    def _():
        for c in own_right():
            c.wait_send()

    def finish(shard, _):
        @pl.when(passes_on(shard))
        def _():
            for c in forward(shard):
                c.wait_send()

        out_copy(shard).wait()
        return 0

    lax.fori_loop(0, n, finish, 0)
    sides[...] = sbuf[...]
    if swaps:
        swap_move(of_first).wait()
    for slot in range(min(2, n)):
        put(0, slot).wait()


def gather_product(x, side, w, w_other, layer, n, transposed, collective_id, swap=None):
    rows, depth = x.shape
    width = w.shape[0] if transposed else w.shape[1]
    tile = min(512 if transposed else 768, width)
    dma = pltpu.SemaphoreType.DMA
    extra = () if swap is None else tuple(swap)
    return pl.pallas_call(
        functools.partial(gather_kernel, n, transposed, tile, layer, swap is not None),
        in_specs=[VM, VM, ANY, ANY] + [ANY] * len(extra),
        out_specs=[ANY, VM, ANY] + [ANY] * min(1, len(extra)),
        out_shape=[
            jax.ShapeDtypeStruct((n * rows, depth), bf16),
            jax.ShapeDtypeStruct((n,) + side.shape, f32),
            jax.ShapeDtypeStruct((n * rows, width), f32),
        ]
        + [jax.ShapeDtypeStruct(v.shape, v.dtype) for v in extra[:1]],
        scratch_shapes=[
            pltpu.VMEM((n, rows, depth), bf16),
            pltpu.VMEM((n,) + side.shape, f32),
            pltpu.VMEM(w.shape, bf16),
            pltpu.VMEM((2, rows, width), f32),
            dma((2, 2)),
            dma((n, 2)),
            dma((n, 2)),
            dma((2,)),
            dma((n,)),
            dma((n,)),
            dma,
            dma((n,)),
            dma((2,)),
        ]
        + [dma, dma] * min(1, len(extra)),
        compiler_params=pltpu.CompilerParams(collective_id=collective_id, has_side_effects=True),
        cost_estimate=pl.CostEstimate(flops=2 * n * rows * depth * width, bytes_accessed=10**8, transcendentals=0),
        name="gather_product",
    )(x, side, w, w_other, *extra)


def scatter_kernel(n, transposed, tile, with_side, layer, works, *refs):
    a, side, w, w_other = refs[:4]
    refs = refs[4:]
    if with_side:
        gain, refs = refs[0], refs[1:]
    if works:
        lhs, rhs, results = (refs[0], refs[1]), refs[2], (refs[5], refs[6])
        refs = refs[3:5] + refs[7:]
    out, side_out, right, left, sbuf, wv, part = refs[:7]
    right_send, right_recv, left_send, left_recv, s_send, s_recv, w_sem = refs[7:14]
    if with_side:
        inv_col, av = refs[14:]
    if works:
        lv, rv, stage, l_sem, r_sem, o_sem = refs[14:]
    m = lax.axis_index("mp")
    rows, width = out.shape
    load = load_weight(layer, w, w_other, wv, w_sem)
    if works:
        rhs_load = pltpu.make_async_copy(rhs, rv, r_sem)
        rhs_load.start()
        first_tiles = lhs[0].shape[1] // 256
        tiles = first_tiles + lhs[1].shape[1] // 256

        def lhs_copy(source, index, slot):
            cols = pl.ds(pl.multiple_of(index * 256, 256), 256)
            return pltpu.make_async_copy(source.at[:, cols], lv.at[slot], l_sem.at[slot])

        def start_lhs(tile_id):
            slot = lax.rem(tile_id, 2)

            @pl.when(tile_id < first_tiles)
            def _():
                lhs_copy(lhs[0], tile_id, slot).start()

            @pl.when(jnp.logical_and(tile_id >= first_tiles, tile_id < tiles))
            def _():
                lhs_copy(lhs[1], tile_id - first_tiles, slot).start()

        def result_copy(which, index, slot):
            span = pl.ds(pl.multiple_of(index * 256, 256), 256)
            columns = results[which].shape[1]
            return pltpu.make_async_copy(stage.at[slot, :, pl.ds(0, columns)], results[which].at[span], o_sem.at[slot])

        def wait_result(tile_id):
            slot = lax.rem(tile_id, 2)

            @pl.when(jnp.logical_and(tile_id >= 0, tile_id < first_tiles))
            def _():
                result_copy(0, 0, slot).wait()

            @pl.when(tile_id >= first_tiles)
            def _():
                result_copy(1, 0, slot).wait()

        def work_product(values, which, index, slot):
            columns = results[which].shape[1]
            span = min(512, columns)

            def column(i, _):
                cols = pl.ds(pl.multiple_of(i * span, span), span)
                stage[slot, :, cols] = mm(lv[slot], values[:, cols], TN).astype(bf16)
                return 0

            lax.fori_loop(0, columns // span, column, 0)
            if columns % span:
                cols = pl.ds(columns - columns % span, columns % span)
                stage[slot, :, cols] = mm(lv[slot], values[:, cols], TN).astype(bf16)
            result_copy(which, index, slot).start()

        def work(tile_id, _):
            slot = lax.rem(tile_id, 2)
            lhs_copy(lhs[0], 0, slot).wait()
            start_lhs(tile_id + 1)
            wait_result(tile_id - 2)

            @pl.when(tile_id < first_tiles)
            def _():
                work_product(a, 0, tile_id, slot)

            @pl.when(tile_id >= first_tiles)
            def _():
                work_product(rv, 1, tile_id - first_tiles, slot)

            return 0

        share = -(-tiles // max(1, n - 1))

        def work_slot(index):
            lax.fori_loop(jnp.minimum(index * share, tiles), jnp.minimum((index + 1) * share, tiles), work, 0)

        start_lhs(jnp.int32(0))
    peers = others("mp", n)
    if with_side:
        greet([at(mp=j) for j in peers])
    else:
        line_barrier(n)
    side_moves = []
    if with_side:
        for i, j in enumerate(peers):
            c = send(side, sbuf.at[m], s_send.at[i], s_recv.at[i], at(mp=j))
            c.start()
            side_moves.append(c)
        sbuf[m] = side[...]
        for c in side_moves:
            c.wait()
        total = sbuf[0]
        for j in range(1, n):
            total = total + sbuf[j]
        inverse = lax.rsqrt(total / (a.shape[1] * n) + epsilon)
        for b in range(side.shape[0]):
            inv_col[b * BLOCK : (b + 1) * BLOCK, :] = jnp.transpose(jnp.broadcast_to(inverse[b], (8, BLOCK)))
        own_rows = pl.ds(pl.multiple_of(m * rows, rows), rows)
        side_out[...] = inv_col[own_rows, :]
    load.wait()
    if works:
        rhs_load.wait()

    def product(j):
        lines = pl.ds(pl.multiple_of(j * rows, rows), rows)
        if with_side:
            av[...] = (a[lines, :] * inv_col[lines, 0:1] * gain[...]).astype(bf16)

        def column(i, _):
            cols = pl.ds(pl.multiple_of(i * tile, tile), tile)
            block = av[...] if with_side else a[lines, :]
            if transposed:
                part[:, cols] = mm(block, wv[cols, :], NT)
            else:
                part[:, cols] = mm(block, wv[:, cols], NN)
            return 0

        lax.fori_loop(0, width // tile, column, 0)

    parts = right_send.shape[1]
    cut = [pl.ds(i * (rows // parts), rows // parts) for i in range(parts)]

    def right_move(j, i):
        return send(right.at[j, cut[i]], right.at[j, cut[i]], right_send.at[j, i], right_recv.at[j, i], at(mp=jnp.minimum(m + 1, n - 1)))

    def left_move(j, i):
        return send(left.at[j, cut[i]], left.at[j, cut[i]], left_send.at[j, i], left_recv.at[j, i], at(mp=jnp.maximum(m - 1, 0)))

    lead = pick(n - 1 - m > m, n - 1 - 2 * m, 2 * m - (n - 1))
    right_major = n - 1 - m >= m

    def body(p, _):
        q = p - lead
        early = p < lead
        major = jnp.logical_or(early, lax.rem(q + 2 * n, 2) == 0)
        k = pick(early, p, pick(major, lead + (q + 2 * n) // 2 - n, (q + 2 * n) // 2 - n))
        to_right = major == right_major
        j = pick(to_right, n - 1 - k, k)
        if works:

            @pl.when(p > 0)
            def _():
                work_slot(p - 1)

        product(j)

        @pl.when(to_right)
        def _():
            for i, c in enumerate(cut):

                @pl.when(m > 0)
                def _():
                    right_move(j, i).wait_recv()
                    right[j, c] = (part[c, :] + right[j, c].astype(f32)).astype(bf16)

                @pl.when(m == 0)
                def _():
                    right[j, c] = part[c, :].astype(bf16)

                right_move(j, i).start()

        @pl.when(jnp.logical_not(to_right))
        def _():
            for i, c in enumerate(cut):

                @pl.when(m < n - 1)
                def _():
                    left_move(j, i).wait_recv()
                    left[j, c] = (part[c, :] + left[j, c].astype(f32)).astype(bf16)

                @pl.when(m == n - 1)
                def _():
                    left[j, c] = part[c, :].astype(bf16)

                left_move(j, i).start()

        return 0

    lax.fori_loop(0, n - 1, body, 0)
    if works:
        work_slot(jnp.int32(n - 2))
    product(m)

    for i, c in enumerate(cut):

        @pl.when(m > 0)
        def _():
            right_move(m, i).wait_recv()
            part[c, :] = part[c, :] + right[m, c].astype(f32)

        @pl.when(m < n - 1)
        def _():
            left_move(m, i).wait_recv()
            part[c, :] = part[c, :] + left[m, c].astype(f32)

    out[...] = part[...]
    if not with_side:
        side_out[...] = jnp.zeros_like(side_out)

    def finish(j, _):
        @pl.when(j > m)
        def _():
            for i in range(parts):
                right_move(j, i).wait_send()

        @pl.when(j < m)
        def _():
            for i in range(parts):
                left_move(j, i).wait_send()

        return 0

    lax.fori_loop(0, n, finish, 0)
    if works:
        for last in range(max(0, tiles - 2), tiles):
            wait_result(jnp.int32(last))


def product_scatter(a, side, w, w_other, layer, n, transposed, collective_id, works=None, gain=None):
    rows = a.shape[0] // n
    width = w.shape[0] if transposed else w.shape[1]
    with_side = side is not None
    if side is None:
        side = jnp.zeros((1, 1, 128), f32)
    tile = 512
    dma = pltpu.SemaphoreType.DMA
    extra, extra_out, extra_scratch = (), [], []
    gains = (gain,) if with_side else ()
    if works is not None:
        (left_one, left_two), rhs = works
        extra = (left_one, left_two, rhs)
        extra_out = [
            jax.ShapeDtypeStruct((left_one.shape[1], a.shape[1]), bf16),
            jax.ShapeDtypeStruct((left_two.shape[1], rhs.shape[1]), bf16),
        ]
        extra_scratch = [
            pltpu.VMEM((2, a.shape[0], 256), bf16),
            pltpu.VMEM(rhs.shape, bf16),
            pltpu.VMEM((2, 256, max(a.shape[1], rhs.shape[1])), bf16),
            dma((2,)),
            dma,
            dma((2,)),
        ]
    result = pl.pallas_call(
        functools.partial(scatter_kernel, n, transposed, tile, with_side, layer, works is not None),
        in_specs=[VM, VM, ANY, ANY] + [VM] * len(gains) + [ANY] * len(extra),
        out_specs=[VM, VM] + [ANY] * len(extra_out),
        out_shape=[
            jax.ShapeDtypeStruct((rows, width), f32),
            jax.ShapeDtypeStruct((rows, 8) if with_side else (8, 128), f32),
        ]
        + extra_out,
        scratch_shapes=[
            pltpu.VMEM((n, rows, width), bf16),
            pltpu.VMEM((n, rows, width), bf16),
            pltpu.VMEM((n,) + side.shape, f32),
            pltpu.VMEM(w.shape, bf16),
            pltpu.VMEM((rows, width), f32),
            dma((n, 2)),
            dma((n, 2)),
            dma((n, 2)),
            dma((n, 2)),
            dma((n,)),
            dma((n,)),
            dma,
        ]
        + extra_scratch
        + ([pltpu.VMEM((a.shape[0], 8), f32), pltpu.VMEM((rows, a.shape[1]), bf16)] if with_side else []),
        compiler_params=pltpu.CompilerParams(collective_id=collective_id, has_side_effects=True),
        cost_estimate=pl.CostEstimate(flops=2 * a.size * width, bytes_accessed=10**8, transcendentals=0),
        name="product_scatter",
    )(a, side, w, w_other, *gains, *extra)
    return result


def start_kernel(sizes, rows_all, w_raw, w_state, w_step, w_out, norm_gain, taps_inner, taps_state, bias, decay, skip, gate_gain,
                 gathered, w0, w1, out_quarter, gn0, gn1, taps0, taps1, heads0, heads1, gg0, gg1,
                 xv, buf, own, other, raw, state, step_all, step_sq, gn_recv, pack, pack_recv,
                 x_sem, raw_sem, st_sem, p_send, p_recv, y_send, y_recv, f_send, f_recv, q_send, q_recv,
                 zo_send, zf_send, z_recv, g_sem, wo_sem, wr_sem):
    inner, state_width, heads, n = sizes
    section, d, m = lax.axis_index("section"), lax.axis_index("dp"), lax.axis_index("mp")
    core = d + 1 - 2 * lax.rem(d, 2)
    far = lax.rem(d + 2, 4)
    core_far = lax.rem(core + 2, 4)
    to_core, to_far, to_section = at(dp=core), at(dp=far), at(section=1 - section)
    has_left, has_right = m > 0, m < n - 1
    depth, width = w0.shape
    quarter = depth // 4
    chunk = min(128, quarter)
    chunks = quarter // chunk
    order = [(0, c) for c in range(chunks)] + [(k, c) for k in (1, 2, 3) for c in range(chunks)]
    owner = [d, core, far, core_far]
    rows = xv.shape[0]

    x_load = pltpu.make_async_copy(rows_all.at[section], xv, x_sem)
    x_load.start()
    step_load = pltpu.make_async_copy(w_step, step_all, st_sem.at[2])
    step_load.start()

    def lines(k, c):
        return pl.ds(pl.multiple_of(owner[k] * quarter + c * chunk, chunk), chunk)

    def raw_loads(i):
        k, c = order[i]
        slot = i % 2
        return (
            pltpu.make_async_copy(w_raw.at[lines(k, c)], raw.at[slot], raw_sem.at[slot]),
            pltpu.make_async_copy(w_state.at[lines(k, c)], state.at[slot], st_sem.at[slot]),
        )

    for g in raw_loads(0):
        g.start()

    barrier = pltpu.get_barrier_semaphore()
    for peer in (to_section, to_core, to_far):
        pl.semaphore_signal(barrier, inc=1, device_id=peer, device_id_type=MESH)

    @pl.when(has_left)
    def _():
        pl.semaphore_signal(barrier, inc=1, device_id=at(mp=m - 1), device_id_type=MESH)

    @pl.when(has_right)
    def _():
        pl.semaphore_signal(barrier, inc=1, device_id=at(mp=m + 1), device_id_type=MESH)

    pack[...] = jnp.zeros_like(pack)
    pack[0:4, 0:inner] = taps_inner[...]
    pack[0:4, inner:] = taps_state[...]
    pack[4:5, 0:inner] = gate_gain[...]
    pack[5:6, 0:heads] = bias[...]
    pack[6:7, 0:heads] = decay[...]
    pack[7:8, 0:heads] = skip[...]
    step_sq[...] = jnp.zeros_like(step_sq)
    pl.semaphore_wait(barrier, 3 + pick(has_left, 1, 0) + pick(has_right, 1, 0))

    gn_move = send(norm_gain, gn_recv, p_send.at[0], p_recv.at[0], to_section)
    pack_move = send(pack, pack_recv, p_send.at[1], p_recv.at[1], to_section)
    gn_move.start()
    pack_move.start()
    step_load.wait()

    def relayout(i):
        k, c = order[i]
        slot = i % 2
        if i + 1 < len(order):
            for g in raw_loads(i + 1):
                g.start()
        for g in raw_loads(i):
            g.wait()
        at_row = pl.ds(c * chunk, chunk)
        own[k, at_row, 0:inner] = raw[slot, :, 0, :]
        own[k, at_row, inner : 2 * inner] = raw[slot, :, 1, :]
        own[k, at_row, 2 * inner : 2 * inner + state_width] = state[slot]
        step_sq[0:heads, 0:chunk] = step_all[:, lines(k, c)].astype(f32)
        own[k, at_row, 2 * inner + state_width :] = jnp.transpose(step_sq[...])[0:chunk, :].astype(bf16)

        @pl.when(section == 0)
        def _():
            pltpu.make_async_copy(own.at[k, at_row], w0.at[lines(k, c)], wo_sem.at[i]).start()

        @pl.when(section == 1)
        def _():
            pltpu.make_async_copy(own.at[k, at_row], w1.at[lines(k, c)], wo_sem.at[i]).start()

    def y_move(c):
        at_row = pl.ds(c * chunk, chunk)
        return send(own.at[0, at_row], other.at[0, at_row], y_send.at[c], y_recv.at[c], to_section)

    def forward_move(slot_from, slot_to, where, c, i):
        at_row = pl.ds(c * chunk, chunk)
        return send(other.at[slot_from, at_row], other.at[slot_to, at_row], f_send.at[i, c], f_recv.at[i, c], where)

    out_rows = out_quarter.shape[0]
    out_move = send(
        w_out.at[pl.ds(pl.multiple_of(d * out_rows, 16), out_rows)], out_quarter, q_send, q_recv, to_section
    )

    def keep(k, c):
        at_row = pl.ds(c * chunk, chunk)

        @pl.when(section == 1)
        def _():
            pltpu.make_async_copy(other.at[k, at_row], w0.at[lines(k, c)], wr_sem.at[k, c]).start()

        @pl.when(section == 0)
        def _():
            pltpu.make_async_copy(other.at[k, at_row], w1.at[lines(k, c)], wr_sem.at[k, c]).start()

    def from_section(c):
        y_move(c).wait_recv()
        forward_move(0, 2, to_far, c, 0).start()
        forward_move(0, 1, to_core, c, 1).start()
        keep(0, c)

    def from_far(c):
        forward_move(0, 2, to_far, c, 0).wait_recv()
        forward_move(2, 3, to_core, c, 2).start()
        keep(2, c)

    def from_core(c):
        forward_move(0, 1, to_core, c, 1).wait_recv()
        keep(1, c)
        forward_move(2, 3, to_core, c, 2).wait_recv()
        keep(3, c)

    def z_own(side):
        to = jnp.maximum(m - 1, 0) if side == 0 else jnp.minimum(m + 1, n - 1)
        return send(xv, buf.at[m], zo_send.at[side], z_recv.at[m], at(mp=to))

    def z_forward(shard):
        to = pick(shard < m, jnp.minimum(m + 1, n - 1), jnp.maximum(m - 1, 0))
        return send(buf.at[shard], buf.at[shard], zf_send.at[shard], z_recv.at[shard], at(mp=to))

    def passes_on(shard):
        return pick(shard < m, has_right, jnp.logical_and(has_left, shard > m))

    def z_out(shard):
        return pltpu.make_async_copy(buf.at[shard], gathered.at[pl.ds(pl.multiple_of(shard * rows, rows), rows)], g_sem.at[shard])

    def from_line(p):
        shard = arrival(p, m, n)
        z_forward(shard).wait_recv()

        @pl.when(passes_on(shard))
        def _():
            z_forward(shard).start()

        z_out(shard).start()

    for i in range(chunks):
        relayout(i)
        y_move(i).start()
        if i == 0:
            x_load.wait()
            gn_move.wait()
            gain = jnp.where(section == 0, norm_gain[...], gn_recv[...])
            half = rows // 2
            for j in range(2):
                part = pl.ds(j * half, half)
                v = xv[part, :].astype(f32)
                scale = lax.rsqrt(jnp.mean(v * v, axis=1, keepdims=True) + epsilon)
                xv[part, :] = (v * scale * gain).astype(bf16)

            @pl.when(has_left)
            def _():
                z_own(0).start()

            @pl.when(has_right)
            def _():
                z_own(1).start()

            buf[m] = xv[...]
            z_out(m).start()
    out_move.start()
    rest = list(range(chunks, len(order)))
    batch = -(-len(rest) // 2)
    for i in rest[:batch]:
        relayout(i)

    def leave_rest():
        for i in rest[batch:]:
            relayout(i)
        pack_move.wait()
        for layer, (gn, taps, heads3, gg) in enumerate(((gn0, taps0, heads0, gg0), (gn1, taps1, heads1, gg1))):
            mine = section == layer
            gn[...] = jnp.where(mine, norm_gain[...], gn_recv[...])
            taps[...] = jnp.where(mine, pack[0:4, :], pack_recv[0:4, :])
            gg[...] = jnp.where(mine, pack[4:5, 0:inner], pack_recv[4:5, 0:inner])
            heads3[...] = jnp.where(mine, pack[5:8, 0:heads], pack_recv[5:8, 0:heads])

    line_steps = list(range(1, n))
    total = chunks + 2
    for c in range(total):
        if c < chunks:
            from_section(c)
        if c == 0:
            leave_rest()
        share = -(-len(line_steps) // (total - 1 - c)) if c < total - 1 else len(line_steps)
        if c > 0:
            for p in line_steps[: 1 if n <= 4 else share]:
                from_line(p)
            line_steps = line_steps[1 if n <= 4 else share :]
        if 0 <= c - 1 < chunks:
            from_far(c - 1)
        if 0 <= c - 2 < chunks:
            from_core(c - 2)
    for p in line_steps:
        from_line(p)
    out_move.wait()
    for c in range(chunks):
        y_move(c).wait_send()
        forward_move(0, 2, to_far, c, 0).wait_send()
        forward_move(0, 1, to_core, c, 1).wait_send()
        forward_move(2, 3, to_core, c, 2).wait_send()
        for k in range(4):
            pltpu.make_async_copy(other.at[k, pl.ds(c * chunk, chunk)], w0.at[lines(k, c)], wr_sem.at[k, c]).wait()
    for i in range(len(order)):
        k, c = order[i]
        pltpu.make_async_copy(own.at[k, pl.ds(c * chunk, chunk)], w0.at[lines(k, c)], wo_sem.at[i]).wait()

    @pl.when(has_left)
    def _():
        z_own(0).wait_send()

    @pl.when(has_right)
    def _():
        z_own(1).wait_send()

    def finish(shard, _):
        @pl.when(jnp.logical_and(shard != m, passes_on(shard)))
        def _():
            z_forward(shard).wait_send()

        z_out(shard).wait()
        return 0

    lax.fori_loop(0, n, finish, 0)


def start_all(rows_all, in_weight, state_weight, step_weight, out_weight, smalls, n):
    depth, _, inner = in_weight.shape
    state_width = state_weight.shape[1]
    heads = step_weight.shape[0]
    rows = rows_all.shape[1]
    used = 2 * inner + state_width + heads
    width = -(-used // 128) * 128
    quarter = depth // 4
    chunk = min(128, quarter)
    chunks = quarter // chunk
    out_rows = out_weight.shape[0] // 4
    taps_width = inner + state_width
    dma = pltpu.SemaphoreType.DMA
    shapes = [
        jax.ShapeDtypeStruct((n * rows, depth), bf16),
        jax.ShapeDtypeStruct((depth, width), bf16),
        jax.ShapeDtypeStruct((depth, width), bf16),
        jax.ShapeDtypeStruct((out_rows, out_weight.shape[1]), bf16),
    ]
    for shape in ((1, depth), (4, taps_width), (3, heads), (1, inner)):
        shapes += [jax.ShapeDtypeStruct(shape, f32)] * 2
    return pl.pallas_call(
        functools.partial(start_kernel, (inner, state_width, heads, n)),
        in_specs=[ANY] * 5 + [VM] * 7,
        out_specs=[ANY] * 4 + [VM] * 8,
        out_shape=shapes,
        scratch_shapes=[
            pltpu.VMEM((rows, depth), bf16),
            pltpu.VMEM((n, rows, depth), bf16),
            pltpu.VMEM((4, quarter, width), bf16),
            pltpu.VMEM((4, quarter, width), bf16),
            pltpu.VMEM((2, chunk, 2, inner), bf16),
            pltpu.VMEM((2, chunk, state_width), bf16),
            pltpu.VMEM((heads, depth), bf16),
            pltpu.VMEM((128, 128), f32),
            pltpu.VMEM((1, depth), f32),
            pltpu.VMEM((8, taps_width), f32),
            pltpu.VMEM((8, taps_width), f32),
            dma,
            dma((2,)),
            dma((3,)),
            dma((2,)),
            dma((2,)),
            dma((chunks,)),
            dma((chunks,)),
            dma((3, chunks)),
            dma((3, chunks)),
            dma,
            dma,
            dma((2,)),
            dma((n,)),
            dma((n,)),
            dma((n,)),
            dma((4 * chunks,)),
            dma((4, chunks)),
        ],
        compiler_params=pltpu.CompilerParams(collective_id=7, has_side_effects=True),
        cost_estimate=pl.CostEstimate(flops=10**7, bytes_accessed=2 * 10**8, transcendentals=0),
        name="start_all",
    )(rows_all, in_weight, state_weight, step_weight, out_weight, *smalls)


def on_device(
    block_input,
    out_grad,
    lengths,
    norm_gain,
    in_weight,
    state_weight,
    step_weight,
    conv_inner,
    conv_state,
    step_bias,
    decay_log,
    skip_gain,
    gate_gain,
    out_weight,
):
    sections = lax.axis_size("section")
    section_id = lax.axis_index("section")
    dp_count = lax.axis_size("dp")
    dp_index = lax.axis_index("dp")
    part_count = lax.axis_size("mp")
    part_index = lax.axis_index("mp")
    row_count, model_width = block_input.shape[2:]
    inner_local = in_weight.shape[3]
    inner_total = inner_local * part_count
    state_width = state_weight.shape[2]
    heads_local = step_weight.shape[2]
    first = section_id == 0
    swap = [(0, 1), (1, 0)]

    rows_in = lax.dynamic_index_in_dim(block_input[:, 0], section_id, 0, keepdims=False)
    outer_grad = lax.dynamic_index_in_dim(out_grad[:, 0], section_id, 0, keepdims=False)
    live = lax.dynamic_index_in_dim(lengths[:, 0], section_id, 0, keepdims=False)
    positions = part_index * row_count + jnp.arange(row_count, dtype=jnp.int32)
    mask = (positions < live).astype(f32)[:, None]

    started = start_all(
        block_input[:, 0],
        in_weight[0],
        state_weight[0],
        step_weight[0].swapaxes(0, 1),
        out_weight[0],
        (norm_gain, conv_inner[0], conv_state[0], step_bias, decay_log, skip_gain, gate_gain),
        part_count,
    )
    first_gathered, w_first, w_second, out_given = started[:4]
    weights = (w_first, w_second)
    smalls = [tuple(started[4 + 2 * i + layer] for i in range(4)) for layer in range(2)]
    own_out = out_weight[0]
    other_out = lax.all_gather(out_given, "dp", axis=0, tiled=True)
    at_inner, at_state, at_step = inner_local, 2 * inner_local, 2 * inner_local + state_width

    counts = (sections, dp_count, part_count)

    def forward(layer, values):
        w_in = weights[layer]
        gain_norm, taps, heads3, gain_gate = smalls[layer]
        row_scale = lax.rsqrt(jnp.mean(values * values, axis=1, keepdims=True) + epsilon)
        if layer == 0:
            gathered = first_gathered
            pre = jnp.dot(gathered, w_in, preferred_element_type=f32)
        else:
            normal = (values * row_scale * gain_norm).astype(bf16)
            gathered, _, pre = gather_product(normal, jnp.zeros((8, 128), f32), w_in, w_in, None, part_count, False, 3)
        mixed, gated, sq, states = mix_forward(pre, taps, heads3, inner_local, state_width, heads_local)
        branch, inverse = product_scatter(
            gated, sq, own_out, other_out, layer, part_count, False, 4 + 6 * layer, gain=gain_gate
        )
        inv_rms = inverse[:, :1]
        result = (values + mask * branch).astype(bf16)
        return result, (values, row_scale, gathered, pre, mixed, states, inv_rms, branch)

    def over_dp(part):
        return lax.psum_scatter(part.astype(bf16), "dp", scatter_dimension=0, tiled=True)

    def summed_rows(left, right):
        return jnp.einsum("ld,lc->dc", left, right, preferred_element_type=f32).astype(bf16)

    def backward(layer, kept, grad, swap, given=None):
        w_in = weights[layer]
        gain_norm, taps, heads3, gain_gate = smalls[layer]
        values, row_scale, gathered, pre, mixed, states, inv_own, branch = kept
        branch_grad = (mask * grad).astype(bf16)
        pull_own = inv_own * inv_own * jnp.sum(branch_grad.astype(f32) * branch, axis=1, keepdims=True) / inner_total
        side = jnp.concatenate([inv_own.reshape(1, -1), pull_own.reshape(1, -1), jnp.zeros((6, row_count), f32)])
        full_grad, sides, normed_grad, theirs = gather_product(
            branch_grad, side, own_out, other_out, layer, part_count, True, 5 + 6 * layer, swap
        )
        scalars = sides[:, :2].transpose(0, 2, 1).reshape(-1, 2)
        normed, dgate, dy, g_gain = gate_backward(pre, mixed, normed_grad, scalars, gain_gate, inner_local)
        if layer == 0:
            out_part = summed_rows(normed, full_grad)
            gate_part = summed_rows(gathered, dgate)
            dy, out_part, gate_part, given = lax.optimization_barrier((dy, out_part, gate_part, given))
            out_part, gate_part = over_dp(out_part), over_dp(gate_part)
        own_grad, g_taps, g_heads = mix_backward(pre, dgate, dy, states, taps, heads3, inner_local, state_width, heads_local)
        if layer == 0:
            rest = summed_rows(gathered, own_grad[:, inner_local:])
            part = jnp.einsum("lc,dc->ld", own_grad, w_in, preferred_element_type=f32).astype(bf16)
            part, rest, out_part, gate_part, given = lax.optimization_barrier((part, rest, out_part, gate_part, given))
            totals = reduce_all(
                [
                    (out_part, given[1], 0, True, None),
                    (gate_part, given[0], 0, True, None),
                    (rest, given[0], inner_local, False, (inner_local, state_width)),
                ],
                counts,
            )
            normal_grad = lax.psum_scatter(part, "mp", scatter_dimension=0, tiled=True)
            normal_grad, totals = lax.optimization_barrier((normal_grad, totals))
            normal_grad = normal_grad.astype(f32)
        else:
            normal_grad, _, in_part, out_part = product_scatter(
                own_grad, None, w_in, w_in, None, part_count, True, 6, ((gathered, normed), full_grad)
            )
            totals = (over_dp(in_part), over_dp(out_part))
        norm_part = jnp.sum(normal_grad * values * row_scale, axis=0)
        scaled_in = normal_grad * gain_norm
        input_grad = (
            grad
            + row_scale * scaled_in
            - values * row_scale**3 * jnp.mean(scaled_in * values, axis=1, keepdims=True)
        )
        own_small = (g_taps[:, :inner_local], g_heads[0, :heads_local], g_heads[1, :heads_local], g_heads[2, :heads_local], g_gain[0])
        common_small = (norm_part, g_taps[:, inner_local:])
        return input_grad, totals, own_small, common_small, theirs

    hidden, kept_first = forward(0, rows_in.astype(f32))
    final, kept_second = forward(1, hidden.astype(f32))
    second_grad, quarters, own_second, common_second, out_theirs = backward(1, kept_second, outer_grad.astype(f32), (final, hidden))
    passed = second_grad.astype(bf16)
    first_grad, totals, own_first, common_first, early = backward(0, kept_first, passed.astype(f32), (passed, passed), quarters)
    out_total, gate_total, rest_total = totals
    late = lax.ppermute(first_grad.astype(bf16), "section", [(1, 0)])

    def flat(first_layer, second_layer):
        v = jnp.concatenate([v.reshape(-1) for v in first_layer + second_layer])
        rows = -(-v.shape[0] // 1024) * 8
        return jnp.pad(v, (0, rows * 128 - v.shape[0])).reshape(rows, 128)

    own_sum, common_sum = small_reduce(flat(own_first, own_second), flat(common_first, common_second), counts)

    def cut(table, pieces):
        sizes = [v.size for v in pieces]
        vector = lax.dynamic_slice_in_dim(table.reshape(-1), section_id * sum(sizes), sum(sizes), 0)
        result, start = [], 0
        for v in pieces:
            result.append(vector[start : start + v.size].reshape((1,) + v.shape))
            start += v.size
        return result

    g_conv_inner, g_bias, g_decay, g_skip, g_gate_gain = cut(own_sum, own_first)
    g_norm, g_conv_state = cut(common_sum, common_first)
    g_in, g_state, g_step = format_grads(gate_total, rest_total, inner_local, state_width, heads_local)

    grad_theirs = jnp.where(first, late, early).astype(f32)

    def by_section(of_first, of_second, theirs):
        mine = jnp.where(first, of_first, of_second)
        return jnp.where(first, jnp.stack([mine, theirs]), jnp.stack([theirs, mine]))[None, :, None]

    return (
        by_section(hidden, final, out_theirs),
        by_section(first_grad, second_grad, grad_theirs),
        g_norm,
        g_in[None],
        g_state[None],
        g_step[None],
        g_conv_inner,
        g_conv_state,
        g_bias,
        g_decay,
        g_skip,
        g_gate_gain,
        out_total.astype(f32)[None],
    )


def solution(mesh):
    return jax.shard_map(
        on_device,
        mesh=mesh,
        in_specs=(
            P(None, "dp", "mp", None),
            P(None, "dp", "mp", None),
            P(None, "dp"),
            P("section", None),
            P("section", None, None, "mp"),
            P("section", None, None),
            P("section", None, "mp"),
            P("section", None, "mp"),
            P("section", None, None),
            P("section", "mp"),
            P("section", "mp"),
            P("section", "mp"),
            P("section", "mp"),
            P("section", "mp", None),
        ),
        out_specs=(
            P("section", None, "dp", "mp", None),
            P("section", None, "dp", "mp", None),
            P("section", None),
            P("section", None, None, "mp"),
            P("section", None, None),
            P("section", None, "mp"),
            P("section", None, "mp"),
            P("section", None, None),
            P("section", "mp"),
            P("section", "mp"),
            P("section", "mp"),
            P("section", "mp"),
            P("section", "mp", None),
        ),
        check_vma=False,
    )
```
